32 devices in a mesh: wave: 16 (over z, x, core), lev: 2 (over y).
Axes of the slice: x: 2, y: 2, z: 4, core: 2. Of those that a mesh axis runs over, the one named last changes fastest.
Arguments:
- spectral: float32 [136, 256, 2562], P('lev', 'wave'), may hold values from -6 to 6
- to_modes: float32 [136, 136], replicated, may hold values from -3 to 3
- from_modes: float32 [136, 136], replicated, may hold values from -3 to 3
- depth: float32 [136], replicated, may hold values from 0.02 to 50
- owner: int32 [128], replicated, may hold values from 0 to 15, as said below
Outputs:
- solved: float32 [136, 128, 2562], P('lev', 'wave')
The draws below stay inside these ranges and needn't reach their ends.
Inputs may be any that keep to these rules, and one draw needn't show every extreme that they name: `owner`: group q holds the pairs q * 1 to q * 1 + 1 - 1; a device stores its groups in increasing q from its first slot on, 1 slots each, and leaves its other slots unused. The 8 groups with the same q // 8 have 8 different owners. A device owns at most 16 groups, and some device exactly that many.
All inputs are finite; a program needn't handle non-finite values.
Results may differ from the reference program's by a relative error of at most 0.000075.
Values sent between devices are 32-bit elements; how exact they have to be, the bound alone decides.
A program may use at most 128 MiB of HBM per device.

```python
import math
import jax
import jax.numpy as jnp
from jax import lax

NT = 1279
LEVELS = 136
KPAIR = 1
GROUPS = 8
PLEN = 1281
CAP = 16
PAIRS = 128
SLOTS = 256
NGROUPS = 128
N_WAVE = 16


def modes_matrix(key, salt):
    base = jax.random.fold_in(key, salt)
    first = jax.random.fold_in(base, 0)
    noise = jnp.clip(jax.random.normal(first, (LEVELS, LEVELS), jnp.float32), -4.0, 4.0)
    matrix = jnp.eye(LEVELS, dtype=jnp.float32) + 0.5 * noise / math.sqrt(LEVELS)
    return matrix


def draw_to_modes(key, part):
    return modes_matrix(key, 31)


def draw_from_modes(key, part):
    return modes_matrix(key, 47)


def draw_owner(key, part):
    first, second = jax.random.split(jax.random.fold_in(key, 11))
    half = N_WAVE // 2
    shifts = jax.random.randint(first, (half,), 0, GROUPS + 1).astype(jnp.int32)
    shifts = shifts.at[0].set(GROUPS)
    counts = jnp.concatenate([GROUPS + shifts, GROUPS - shifts])
    labels = jax.random.permutation(second, N_WAVE).astype(jnp.int32)
    bounds = jnp.cumsum(counts)
    positions = jnp.arange(NGROUPS, dtype=jnp.int32)
    runs = jnp.sum((positions[:, None] >= bounds[None, :]).astype(jnp.int32), axis=1)
    sequence = labels[runs]
    target = positions // GROUPS
    within = positions % GROUPS
    return sequence[within * N_WAVE + target].astype(jnp.int32)


def level_of(stream_key, dims, pieces, low, largest):
    factor_of, own = 1.0, jax.random.fold_in(stream_key, 6)
    for axis_at, parts in pieces:
        steps = jnp.exp(jax.random.uniform(jax.random.fold_in(own, axis_at), (parts,), jnp.float32, low / len(pieces), largest / len(pieces)))
        factor_of = factor_of * jnp.repeat(steps, dims[axis_at] // parts).reshape([-1 if axis == axis_at else 1 for axis in range(len(dims))])
    return factor_of


def scatter_about(own_key, shape, scale, bound, shards=(), kind=jnp.bfloat16):
    result = scale * jax.random.normal(own_key, shape, jnp.float32)
    if shards:
        result = result * level_of(own_key, shape, shards, -0.22, 0.18)
    return jnp.clip(result, -bound, bound).astype(kind)


def setup_inputs(seed: int = 0) -> dict:
    seeds = jax.random.split(jax.random.key(seed), 6)
    return {
        "spectral": scatter_about(seeds[0], (LEVELS, SLOTS, 2 * PLEN), 1.0, 6.0, ((0, 2), (1, 16)), jnp.float32),
        "to_modes": draw_to_modes(jax.random.fold_in(seeds[5], 71), 0),
        "from_modes": draw_from_modes(jax.random.fold_in(seeds[5], 71), 0),
        "depth": jnp.clip(jnp.exp(jax.random.uniform(seeds[3], (LEVELS,), jnp.float32, math.log(0.02), math.log(50.0))), 0.02, 50.0),
        "owner": draw_owner(jax.random.fold_in(seeds[5], 71), 0),
    }


def reference(spectral, to_modes, from_modes, depth, owner):
    numbers = jnp.arange(NGROUPS, dtype=jnp.int32)
    same = owner[:, None] == owner[None, :]
    rank = jnp.sum((same & (numbers[None, :] < numbers[:, None])).astype(jnp.int32), axis=1)
    first = owner * CAP + rank * KPAIR
    source = (first[:, None] + jnp.arange(KPAIR, dtype=jnp.int32)[None, :]).reshape(PAIRS).astype(jnp.int32)
    moved = jnp.take(spectral, source, axis=1)
    flat = moved.reshape(LEVELS, PAIRS * 2 * PLEN)
    pair = jnp.arange(PAIRS, dtype=jnp.int32)[:, None]
    column = jnp.arange(2 * PLEN, dtype=jnp.int32)[None, :]
    within = column % PLEN
    degree = jnp.where(within <= NT - pair, pair + within, within - 1)
    ratio = (degree * (degree + 1)).astype(jnp.float32) / float(NT * (NT + 1))
    ratio = ratio.reshape(PAIRS * 2 * PLEN)
    modes = jnp.dot(to_modes, flat, precision=lax.Precision.HIGHEST, preferred_element_type=jnp.float32)
    scaled = modes / (1.0 + depth[:, None] * ratio[None, :])
    solved = jnp.dot(from_modes, scaled, precision=lax.Precision.HIGHEST, preferred_element_type=jnp.float32)
    return solved.reshape(LEVELS, PAIRS, 2 * PLEN)
```

```python
import functools

import jax
import jax.numpy as jnp
from jax import lax
from jax.experimental import pallas as pl
from jax.experimental.pallas import tpu as pltpu
from jax.sharding import PartitionSpec as P

NT = 1279
KPAIR = 1
LANES = 128
TILES = 3
HEAD = (1, 2, 2)
TAIL = (2, 2, 1, 1)
AHEAD = 2
MESH = pl.DeviceIdType.MESH


def split(whole):
    middle = whole - sum(HEAD) - sum(TAIL)
    if middle < 0:
        return (1,) * whole
    rest = (middle % TILES,) if middle % TILES else ()
    return HEAD + (TILES,) * (middle // TILES) + rest + TAIL


def flipped(index, mask, count):
    result = index * 0
    bit = 1
    while bit < count:
        own = lax.rem(lax.div(index, bit), 2)
        result = result + bit * ((1 - own) if mask & bit else own)
        bit *= 2
    return result


def halves(value):
    high = value.astype(jnp.bfloat16)
    low = (value - high.astype(jnp.float32)).astype(jnp.bfloat16)
    return high, low


def product(left_both, left_high, right, rows):
    high, low = halves(right)
    both = jnp.dot(left_both, high, preferred_element_type=jnp.float32)
    cross = jnp.dot(left_high, low, preferred_element_type=jnp.float32)
    return (both[rows:] + cross) + both[:rows]


def kernel(sizes, picks, places, spectral, last, to_modes, from_modes, depth, solved, *scratch):
    waves, levs, pairs, slots, levels, width, parts, packs, rest = sizes
    chunks = len(parts)
    received, rows_in, sending, mine, theirs, staged = (
        scratch[kind * chunks : (kind + 1) * chunks] for kind in range(6)
    )
    rows_last, tail_sent, tail_got, tail_mine, tail_theirs = scratch[6 * chunks : 6 * chunks + 5]
    to_both, from_both, load_sem, send_sem, recv_sem, lev_send, lev_recv, out_sem = scratch[
        6 * chunks + 5 :
    ]
    me = lax.axis_index("wave")
    lev = lax.axis_index("lev")
    modes_number = depth.shape[0]
    firsts = [sum(parts[:c]) for c in range(chunks)]
    final = chunks - 1

    def load(c, tile):
        number = firsts[c] + tile
        if number < sum(parts):
            source = spectral.at[:, pl.ds(number * LANES, LANES)]
            return pltpu.make_async_copy(source, rows_in[c].at[tile], load_sem.at[number])
        target = rows_last.at[pl.ds(0, levels * slots)]
        return pltpu.make_async_copy(last, target, load_sem.at[number])

    def width_of(c):
        return parts[c] + (1 if c == final else 0)

    for c in range(chunks):
        for tile in range(width_of(c)):
            load(c, tile).start()

    barrier = pltpu.get_barrier_semaphore()
    for mask in range(1, waves):
        pl.semaphore_signal(
            barrier, inc=1, device_id={"wave": flipped(me, mask, waves)}, device_id_type=MESH
        )
    for turn in range(1, levs):
        pl.semaphore_signal(
            barrier, inc=1, device_id={"lev": lax.rem(lev + turn, levs)}, device_id_type=MESH
        )

    for part in range(levs):
        high, low = halves(to_modes[part])
        to_both[part, :modes_number] = high
        to_both[part, modes_number:] = low
    high, low = halves(from_modes[...])
    from_both[0], from_both[1] = high, low
    pl.semaphore_wait(barrier, waves + levs - 2)

    def packed(slot):
        lane = lax.broadcasted_iota(jnp.int32, (8, LANES), 1)
        total = rows_last[pl.ds(slot, 8, stride=slots), :]
        for k in range(1, packs):
            block = rows_last[pl.ds(8 * k * slots + slot, 8, stride=slots), :]
            total = jnp.where(lane >= k * rest, pltpu.roll(block, k * rest, 1), total)
        return total

    def unpacked(block):
        pieces = [block] + [pltpu.roll(block, LANES - k * rest, 1) for k in range(1, packs)]
        return jnp.concatenate(pieces, axis=0)[:levels]

    def send(c):
        for tile in range(width_of(c)):
            load(c, tile).wait()

        def pick(mask, target):
            slot = picks[flipped(me, mask, waves)]
            for tile in range(parts[c]):
                target[:, pl.ds(tile * LANES, LANES)] = rows_in[c][
                    tile, pl.ds(slot, levels, stride=slots), :
                ]

        def push(mask, source, target, number):
            pltpu.make_async_remote_copy(
                src_ref=source.at[mask - 1],
                dst_ref=target.at[mask],
                send_sem=send_sem.at[number],
                recv_sem=recv_sem.at[number],
                device_id={"wave": flipped(me, mask, waves)},
                device_id_type=MESH,
            ).start()

        if c == final:
            for mask in range(waves - 1, 0, -1):
                tail_sent[mask - 1] = packed(picks[flipped(me, mask, waves)])
                push(mask, tail_sent, tail_got, chunks)
            tail_got[0] = packed(picks[me])
        for mask in range(waves - 1, 0, -1):
            pick(mask, sending[c].at[mask - 1])
            push(mask, sending[c], received[c], c)
        pick(0, received[c].at[0])

    def lev_copy(c, turn):
        source, target = (tail_mine, tail_theirs) if c == chunks else (mine[c], theirs[c])
        return pltpu.make_async_remote_copy(
            src_ref=source,
            dst_ref=target.at[turn - 1],
            send_sem=lev_send.at[c, turn - 1],
            recv_sem=lev_recv.at[c, turn - 1],
            device_id={"lev": lax.rem(lev + turn, levs)},
            device_id_type=MESH,
        )

    def out_copy(c, tile):
        number = firsts[c] + tile
        columns = solved.at[:, pl.ds(number * LANES, LANES)]
        return pltpu.make_async_copy(staged[c].at[tile], columns, out_sem.at[number])

    def gather(c):
        if c == final:
            arrived = tail_got.at[pl.ds(1, waves - 1)]
            pltpu.make_async_copy(arrived, arrived, recv_sem.at[chunks]).wait()
            for pair in range(pairs):
                tail_mine[pair] = tail_got[places[pair]]
            for turn in range(1, levs):
                lev_copy(chunks, turn).start()
        arrived = received[c].at[pl.ds(1, waves - 1)]
        pltpu.make_async_copy(arrived, arrived, recv_sem.at[c]).wait()

        @pl.loop(0, pairs)
        def _(pair):
            mine[c][pair] = received[c][places[pair]]

        for turn in range(1, levs):
            lev_copy(c, turn).start()

    def solve(c):
        for turn in range(1, levs):
            lev_copy(c, turn).wait_recv()
            if c == final:
                lev_copy(chunks, turn).wait_recv()
        size = width_of(c) * LANES
        column = lax.broadcasted_iota(jnp.int32, (1, size), 1) + firsts[c] * LANES
        within = jnp.where(column >= width // 2, column - width // 2, column)

        @pl.loop(0, pairs)
        def _(pair):
            wavenumber = me * pairs + pair
            degree = jnp.where(within <= NT - wavenumber, wavenumber + within, within - 1)
            ratio = (degree * (degree + 1)).astype(jnp.float32) / float(NT * (NT + 1))
            modes = None
            for turn in range(levs):
                source = lax.rem(lev + levs - turn, levs)
                block = mine[c][pair] if turn == 0 else theirs[c][turn - 1, pair]
                if c == final:
                    tail = tail_mine[pair] if turn == 0 else tail_theirs[turn - 1, pair]
                    block = jnp.concatenate([block, unpacked(tail)], axis=1)
                matrix = to_both.at[source]
                term = product(matrix[...], matrix[:modes_number], block, modes_number)
                modes = term if modes is None else modes + term
            scaled = modes / (1.0 + depth[...] * ratio)
            high, low = halves(scaled)
            from_high = from_both[0]
            result = jnp.dot(from_both[1], high, preferred_element_type=jnp.float32)
            result += jnp.dot(from_high, low, preferred_element_type=jnp.float32)
            result += jnp.dot(from_high, high, preferred_element_type=jnp.float32)
            for tile in range(width_of(c)):
                staged[c][tile, pl.ds(pair, levels, stride=pairs), :] = result[
                    :, tile * LANES : (tile + 1) * LANES
                ]

        for tile in range(width_of(c)):
            out_copy(c, tile).start()

    for c in range(min(AHEAD, chunks)):
        send(c)
    for c in range(chunks):
        if c + AHEAD < chunks:
            send(c + AHEAD)
        gather(c)
        if c >= 1:
            solve(c - 1)
    solve(final)
    for c in range(chunks + 1):
        sent = tail_sent if c == chunks else sending[c]
        pltpu.make_async_copy(sent, sent, send_sem.at[c]).wait()
        for turn in range(1, levs):
            lev_copy(c, turn).wait_send()
    for c in range(chunks):
        for tile in range(width_of(c)):
            out_copy(c, tile).wait()


def per_device(spectral, to_modes, from_modes, depth, owner):
    waves, levs = lax.axis_size("wave"), lax.axis_size("lev")
    levels, slots, width = spectral.shape
    groups = owner.shape[0] // waves
    pairs = groups * KPAIR
    modes_number = depth.shape[0]
    own_index, lev_index = lax.axis_index("wave"), lax.axis_index("lev")
    numbers = jnp.arange(owner.shape[0], dtype=jnp.int32)
    mine = owner == own_index
    before = (numbers[:, None] > numbers[None, :]) & mine[None, :]
    rank = jnp.sum(before.astype(jnp.int32), axis=1)
    picks = jnp.sum(jnp.where(mine, rank, 0).reshape(waves, groups), axis=1)
    places = lax.dynamic_slice_in_dim(owner, own_index * groups, groups) ^ own_index
    whole, rest = width // LANES, width % LANES
    packs = pl.cdiv(levels, 8)
    assert 0 < rest and packs * rest <= LANES
    parts = split(whole)
    chunks = len(parts)
    sizes = (waves, levs, pairs, slots, levels, width, parts, packs, rest)
    rows = spectral.reshape(levels * slots, width)
    last = jnp.pad(rows[:, whole * LANES :], ((0, 0), (0, LANES - rest)))
    by_lev = to_modes.reshape(modes_number, levs, levels).transpose(1, 0, 2)
    own_rows = lax.dynamic_slice_in_dim(from_modes, lev_index * levels, levels)
    vmem, smem, anywhere = (
        pl.BlockSpec(memory_space=space) for space in (pltpu.VMEM, pltpu.SMEM, pl.ANY)
    )
    dma = pltpu.SemaphoreType.DMA
    f32, bf16 = jnp.float32, jnp.bfloat16
    widths = [tiles * LANES for tiles in parts]
    staged_tiles = parts[:-1] + (parts[-1] + 1,)
    solved = pl.pallas_call(
        functools.partial(kernel, sizes),
        out_shape=jax.ShapeDtypeStruct((levels * pairs, (whole + 1) * LANES), f32),
        in_specs=[smem, smem, anywhere, anywhere, vmem, vmem, vmem],
        out_specs=anywhere,
        scratch_shapes=[pltpu.VMEM((waves, levels, size), f32) for size in widths]
        + [pltpu.VMEM((tiles, levels * slots, LANES), f32) for tiles in parts]
        + [pltpu.VMEM((waves - 1, levels, size), f32) for size in widths]
        + [pltpu.VMEM((pairs, levels, size), f32) for size in widths]
        + [pltpu.VMEM((levs - 1, pairs, levels, size), f32) for size in widths]
        + [pltpu.VMEM((tiles, levels * pairs, LANES), f32) for tiles in staged_tiles]
        + [
            pltpu.VMEM((8 * packs * slots, LANES), f32),
            pltpu.VMEM((waves - 1, 8, LANES), f32),
            pltpu.VMEM((waves, 8, LANES), f32),
            pltpu.VMEM((pairs, 8, LANES), f32),
            pltpu.VMEM((levs - 1, pairs, 8, LANES), f32),
            pltpu.VMEM((levs, 2 * modes_number, levels), bf16),
            pltpu.VMEM((2, levels, modes_number), bf16),
            dma((whole + 1,)),
            dma((chunks + 1,)),
            dma((chunks + 1,)),
            dma((chunks + 1, levs - 1)),
            dma((chunks + 1, levs - 1)),
            dma((whole + 1,)),
        ],
        compiler_params=pltpu.CompilerParams(
            collective_id=0, has_side_effects=True, vmem_limit_bytes=67043328
        ),
    )(picks, places, rows, last, by_lev, own_rows, depth[:, None])
    return solved.reshape(levels, pairs, (whole + 1) * LANES)[:, :, :width]


def solution(mesh):
    placed = (P("lev", "wave", None), P(), P(), P(), P())
    return jax.shard_map(
        per_device, mesh=mesh, in_specs=placed, out_specs=P("lev", "wave", None), check_vma=False
    )
```

```python
import functools

import jax
import jax.numpy as jnp
from jax import lax
from jax.experimental import pallas as pl
from jax.experimental.pallas import tpu as pltpu
from jax.sharding import PartitionSpec as P

NT = 1279
KPAIR = 1
LANES = 128
TILES = 3
HEAD = (1, 2, 2)
TAIL = (2, 2, 1, 1)
AHEAD = 2
QUAD = 4
RING = 3
LAGS = (0, 1, 2, 3, 4)
MESH = pl.DeviceIdType.MESH


def split(whole):
    middle = whole - sum(HEAD) - sum(TAIL)
    if middle < 0:
        return (1,) * whole
    rest = (middle % TILES,) if middle % TILES else ()
    return HEAD + (TILES,) * (middle // TILES) + rest + TAIL


def flipped(index, mask, count):
    result = index * 0
    bit = 1
    while bit < count:
        own = lax.rem(lax.div(index, bit), 2)
        result = result + bit * ((1 - own) if mask & bit else own)
        bit *= 2
    return result


def halves(value):
    high = value.astype(jnp.bfloat16)
    low = (value - high.astype(jnp.float32)).astype(jnp.bfloat16)
    return high, low


def product(left_both, left_high, right, rows):
    high, low = halves(right)
    both = jnp.dot(left_both, high, preferred_element_type=jnp.float32)
    cross = jnp.dot(left_high, low, preferred_element_type=jnp.float32)
    return (both[rows:] + cross) + both[:rows]


def kernel(sizes, picks, places, spectral, last, to_modes, from_modes, depth, solved, *scratch):
    waves, levs, pairs, slots, levels, width, parts, packs, rest = sizes
    chunks = len(parts)
    received, rows_in, sending, mine, theirs, staged = (
        scratch[kind * chunks : (kind + 1) * chunks] for kind in range(6)
    )
    rows_last, tail_sent, tail_got, tail_mine, tail_theirs = scratch[6 * chunks : 6 * chunks + 5]
    to_both, from_both, load_sem, send_sem, recv_sem, lev_send, lev_recv, out_sem = scratch[
        6 * chunks + 5 :
    ]
    me = lax.axis_index("wave")
    lev = lax.axis_index("lev")
    modes_number = depth.shape[0]
    firsts = [sum(parts[:c]) for c in range(chunks)]
    final = chunks - 1

    def load(c, tile):
        number = firsts[c] + tile
        if number < sum(parts):
            source = spectral.at[:, pl.ds(number * LANES, LANES)]
            return pltpu.make_async_copy(source, rows_in[c].at[tile], load_sem.at[number])
        target = rows_last.at[pl.ds(0, levels * slots)]
        return pltpu.make_async_copy(last, target, load_sem.at[number])

    def width_of(c):
        return parts[c] + (1 if c == final else 0)

    for c in range(chunks):
        for tile in range(width_of(c)):
            load(c, tile).start()

    barrier = pltpu.get_barrier_semaphore()
    for mask in range(1, waves):
        pl.semaphore_signal(
            barrier, inc=1, device_id={"wave": flipped(me, mask, waves)}, device_id_type=MESH
        )
    for turn in range(1, levs):
        pl.semaphore_signal(
            barrier, inc=1, device_id={"lev": lax.rem(lev + turn, levs)}, device_id_type=MESH
        )

    for part in range(levs):
        high, low = halves(to_modes[part])
        to_both[part, :modes_number] = high
        to_both[part, modes_number:] = low
    high, low = halves(from_modes[...])
    from_both[0], from_both[1] = high, low
    pl.semaphore_wait(barrier, waves + levs - 2)

    def packed(slot):
        lane = lax.broadcasted_iota(jnp.int32, (8, LANES), 1)
        total = rows_last[pl.ds(slot, 8, stride=slots), :]
        for k in range(1, packs):
            block = rows_last[pl.ds(8 * k * slots + slot, 8, stride=slots), :]
            total = jnp.where(lane >= k * rest, pltpu.roll(block, k * rest, 1), total)
        return total

    def unpacked(block):
        pieces = [block] + [pltpu.roll(block, LANES - k * rest, 1) for k in range(1, packs)]
        return jnp.concatenate(pieces, axis=0)[:levels]

    def send(c):
        for tile in range(width_of(c)):
            load(c, tile).wait()

        def pick(mask, target):
            slot = picks[flipped(me, mask, waves)]
            for tile in range(parts[c]):
                target[:, pl.ds(tile * LANES, LANES)] = rows_in[c][
                    tile, pl.ds(slot, levels, stride=slots), :
                ]

        def push(mask, source, target, number):
            pltpu.make_async_remote_copy(
                src_ref=source.at[mask - 1],
                dst_ref=target.at[mask],
                send_sem=send_sem.at[number],
                recv_sem=recv_sem.at[number],
                device_id={"wave": flipped(me, mask, waves)},
                device_id_type=MESH,
            ).start()

        if c == final:
            for mask in range(waves - 1, 0, -1):
                tail_sent[mask - 1] = packed(picks[flipped(me, mask, waves)])
                push(mask, tail_sent, tail_got, chunks)
            tail_got[0] = packed(picks[me])
        for mask in range(waves - 1, 0, -1):
            pick(mask, sending[c].at[mask - 1])
            push(mask, sending[c], received[c], c)
        pick(0, received[c].at[0])

    def lev_copy(c, turn):
        source, target = (tail_mine, tail_theirs) if c == chunks else (mine[c], theirs[c])
        return pltpu.make_async_remote_copy(
            src_ref=source,
            dst_ref=target.at[turn - 1],
            send_sem=lev_send.at[c, turn - 1],
            recv_sem=lev_recv.at[c, turn - 1],
            device_id={"lev": lax.rem(lev + turn, levs)},
            device_id_type=MESH,
        )

    def out_copy(c, tile):
        number = firsts[c] + tile
        columns = solved.at[:, pl.ds(number * LANES, LANES)]
        return pltpu.make_async_copy(staged[c].at[tile], columns, out_sem.at[number])

    def gather(c):
        if c == final:
            arrived = tail_got.at[pl.ds(1, waves - 1)]
            pltpu.make_async_copy(arrived, arrived, recv_sem.at[chunks]).wait()
            for pair in range(pairs):
                tail_mine[pair] = tail_got[places[pair]]
            for turn in range(1, levs):
                lev_copy(chunks, turn).start()
        arrived = received[c].at[pl.ds(1, waves - 1)]
        pltpu.make_async_copy(arrived, arrived, recv_sem.at[c]).wait()

        @pl.loop(0, pairs)
        def _(pair):
            mine[c][pair] = received[c][places[pair]]

        for turn in range(1, levs):
            lev_copy(c, turn).start()

    def solve(c):
        for turn in range(1, levs):
            lev_copy(c, turn).wait_recv()
            if c == final:
                lev_copy(chunks, turn).wait_recv()
        size = width_of(c) * LANES
        column = lax.broadcasted_iota(jnp.int32, (1, size), 1) + firsts[c] * LANES
        within = jnp.where(column >= width // 2, column - width // 2, column)

        @pl.loop(0, pairs)
        def _(pair):
            wavenumber = me * pairs + pair
            degree = jnp.where(within <= NT - wavenumber, wavenumber + within, within - 1)
            ratio = (degree * (degree + 1)).astype(jnp.float32) / float(NT * (NT + 1))
            modes = None
            for turn in range(levs):
                source = lax.rem(lev + levs - turn, levs)
                block = mine[c][pair] if turn == 0 else theirs[c][turn - 1, pair]
                if c == final:
                    tail = tail_mine[pair] if turn == 0 else tail_theirs[turn - 1, pair]
                    block = jnp.concatenate([block, unpacked(tail)], axis=1)
                matrix = to_both.at[source]
                term = product(matrix[...], matrix[:modes_number], block, modes_number)
                modes = term if modes is None else modes + term
            scaled = modes / (1.0 + depth[...] * ratio)
            high, low = halves(scaled)
            from_high = from_both[0]
            result = jnp.dot(from_both[1], high, preferred_element_type=jnp.float32)
            result += jnp.dot(from_high, low, preferred_element_type=jnp.float32)
            result += jnp.dot(from_high, high, preferred_element_type=jnp.float32)
            for tile in range(width_of(c)):
                staged[c][tile, pl.ds(pair, levels, stride=pairs), :] = result[
                    :, tile * LANES : (tile + 1) * LANES
                ]

        for tile in range(width_of(c)):
            out_copy(c, tile).start()

    for c in range(min(AHEAD, chunks)):
        send(c)
    for c in range(chunks):
        if c + AHEAD < chunks:
            send(c + AHEAD)
        gather(c)
        if c >= 1:
            solve(c - 1)
    solve(final)
    for c in range(chunks + 1):
        sent = tail_sent if c == chunks else sending[c]
        pltpu.make_async_copy(sent, sent, send_sem.at[c]).wait()
        for turn in range(1, levs):
            lev_copy(c, turn).wait_send()
    for c in range(chunks):
        for tile in range(width_of(c)):
            out_copy(c, tile).wait()


def relay_kernel(sizes, picks, places, relayed, landed, spectral, last, to_modes, from_modes, depth, solved, *scratch):
    waves, levs, pairs, slots, levels, width, parts, packs, rest, room = sizes
    chunks = len(parts)
    scratch = list(scratch)

    def take(count):
        taken = scratch[:count]
        del scratch[:count]
        return taken

    received, carried, arrived_far, final_far, theirs = (take(chunks) for _ in range(5))
    rows_in, direct_out, carry_out, relay_out, forward_out, mine, staged = (
        take(RING) for _ in range(7)
    )
    rows_last, tail_sent, tail_got, tail_mine, tail_theirs, to_both, from_both = take(7)
    (load_sem, direct_send, direct_recv, carry_send, carry_recv, relay_send, relay_recv,
     forward_send, forward_recv, lev_send, lev_recv, out_sem) = take(12)
    me = lax.axis_index("wave")
    lev = lax.axis_index("lev")
    half = waves // 2
    side = lax.div(me, half)
    step = lax.rem(lax.div(me, QUAD), 2)
    quad = lax.rem(me, QUAD)
    core = lax.rem(me, 2)
    outer = lax.rem(side + step + 1, 2)
    cut = levels // 2 // 8 * 8
    part_rows = levels - cut
    modes_number = depth.shape[0]
    firsts = [sum(parts[:c]) for c in range(chunks)]
    final = chunks - 1

    def ring(buffers, c):
        ref = buffers[c % RING]
        size = parts[c] * LANES
        if ref.shape[-1] == size:
            return ref
        return ref.at[tuple(slice(None) for _ in ref.shape[:-1]) + (pl.ds(0, size),)]

    def to_wave(index):
        return {"wave": index}

    def load(c, tile):
        number = firsts[c] + tile
        if tile < parts[c]:
            source = spectral.at[:, pl.ds(number * LANES, LANES)]
            return pltpu.make_async_copy(source, rows_in[c % RING].at[tile], load_sem.at[number])
        target = rows_last.at[pl.ds(0, levels * slots)]
        return pltpu.make_async_copy(last, target, load_sem.at[number])

    def width_of(c):
        return parts[c] + (1 if c == final else 0)

    def finish(ref, semaphore):
        pltpu.make_async_copy(ref, ref, semaphore).wait()

    def push(source, target, send_sem, recv_sem, index):
        pltpu.make_async_remote_copy(
            src_ref=source,
            dst_ref=target,
            send_sem=send_sem,
            recv_sem=recv_sem,
            device_id=to_wave(index),
            device_id_type=MESH,
        ).start()

    load(final, parts[final]).start()
    for c in range(min(RING, chunks)):
        for tile in range(parts[c]):
            load(c, tile).start()

    barrier = pltpu.get_barrier_semaphore()
    for mask in range(1, waves):
        pl.semaphore_signal(
            barrier, inc=1, device_id=to_wave(flipped(me, mask, waves)), device_id_type=MESH
        )
    for turn in range(1, levs):
        pl.semaphore_signal(
            barrier, inc=1, device_id={"lev": lax.rem(lev + turn, levs)}, device_id_type=MESH
        )
    for part in range(levs):
        high, low = halves(to_modes[part])
        to_both[part, :modes_number] = high
        to_both[part, modes_number:] = low
    high, low = halves(from_modes[...])
    from_both[0], from_both[1] = high, low
    pl.semaphore_wait(barrier, waves + levs - 2)

    def packed(slot):
        lane = lax.broadcasted_iota(jnp.int32, (8, LANES), 1)
        total = rows_last[pl.ds(slot, 8, stride=slots), :]
        for k in range(1, packs):
            block = rows_last[pl.ds(8 * k * slots + slot, 8, stride=slots), :]
            total = jnp.where(lane >= k * rest, pltpu.roll(block, k * rest, 1), total)
        return total

    def unpacked(block):
        pieces = [block] + [pltpu.roll(block, LANES - k * rest, 1) for k in range(1, packs)]
        return jnp.concatenate(pieces, axis=0)[:levels]

    def drain_send(c):
        finish(ring(direct_out, c), direct_send.at[c])
        carry = ring(carry_out, c)

        @pl.when(outer == 1)
        def _():
            finish(carry, carry_send.at[c])

        @pl.when(outer == 0)
        def _():
            finish(carry.at[pl.ds(1, QUAD - 1)], carry_send.at[c])

    def send(c):
        for tile in range(width_of(c)):
            load(c, tile).wait()
        if c >= RING:
            drain_send(c - RING)
        source = rows_in[c % RING]
        carry, direct = ring(carry_out, c), ring(direct_out, c)

        def pick(slot, target, first, count):
            for tile in range(parts[c]):
                target[:, pl.ds(tile * LANES, LANES)] = source[
                    tile, pl.ds(first * slots + slot, count, stride=slots), :
                ]

        for mask in range(QUAD - 1, -1, -1):
            carrier = flipped(quad, mask, QUAD)
            first = lax.rem(carrier, 2) * cut

            @pl.loop(0, QUAD)
            def _(j):
                index = (1 - side) * half + lax.div(j, 2) * QUAD
                index = index + lax.div(carrier, 2) * 2 + lax.rem(j, 2)
                pick(picks[index], carry.at[mask, j], first, part_rows)

            place = (mask + QUAD * outer) * QUAD
            device = side * half + (1 - side) * QUAD + carrier

            def carry_on():
                target = carried[c].at[pl.ds(place, QUAD)]
                push(carry.at[mask], target, carry_send.at[c], carry_recv.at[c], device)

            if mask:
                carry_on()
            else:
                pl.when(outer == 1)(carry_on)

                @pl.when(outer == 0)
                def _():
                    @pl.loop(0, QUAD)
                    def _(j):
                        carried[c][j] = carry[0, j]

        if c == final:
            for mask in range(waves - 1, 0, -1):
                index = flipped(me, mask, waves)
                tail_sent[mask - 1] = packed(picks[index])
                push(
                    tail_sent.at[mask - 1],
                    tail_got.at[mask],
                    direct_send.at[chunks],
                    direct_recv.at[chunks],
                    index,
                )
            tail_got[0] = packed(picks[me])
        for mask in range(half - 1, 0, -1):
            index = flipped(me, mask, waves)
            pick(picks[index], direct.at[mask - 1], 0, levels)
            push(
                direct.at[mask - 1],
                received[c].at[mask],
                direct_send.at[c],
                direct_recv.at[c],
                index,
            )
        pick(picks[me], received[c].at[0], 0, levels)
        if c + RING < chunks:
            for tile in range(parts[c + RING]):
                load(c + RING, tile).start()

    def relay(c):
        @pl.when(outer == 0)
        def _():
            finish(carried[c].at[pl.ds(QUAD, (half - 1) * QUAD)], carry_recv.at[c])
            if c >= RING:
                finish(ring(relay_out, c - RING), relay_send.at[c - RING])
            block = ring(relay_out, c)

            @pl.loop(0, room)
            def _(g):
                block[g] = carried[c][relayed[g]]

            push(
                block, arrived_far[c], relay_send.at[c], relay_recv.at[c],
                flipped(me, 3 * QUAD, waves),
            )

    def forward(c):
        @pl.when(outer == 0)
        def _():
            finish(arrived_far[c], relay_recv.at[c])
            if c >= RING:
                finish(ring(forward_out, c - RING), forward_send.at[c - RING])
            block = ring(forward_out, c)
            for number, mask in enumerate((QUAD + 1, QUAD, 1)):

                @pl.loop(0, pairs)
                def _(pair):
                    block[number, pair] = arrived_far[c][landed[number * pairs + pair]]

                push(
                    block.at[number],
                    final_far[c].at[mask % 2],
                    forward_send.at[c],
                    forward_recv.at[c],
                    flipped(me, mask, waves),
                )

            @pl.loop(0, pairs)
            def _(pair):
                final_far[c][0, pair] = arrived_far[c][landed[3 * pairs + pair]]

    def lev_copy(c, turn):
        source, target = (
            (tail_mine, tail_theirs) if c == chunks else (ring(mine, c), theirs[c])
        )
        return pltpu.make_async_remote_copy(
            src_ref=source,
            dst_ref=target.at[turn - 1],
            send_sem=lev_send.at[c, turn - 1],
            recv_sem=lev_recv.at[c, turn - 1],
            device_id={"lev": lax.rem(lev + turn, levs)},
            device_id_type=MESH,
        )

    def out_copy(c, tile):
        number = firsts[c] + tile
        columns = solved.at[:, pl.ds(number * LANES, LANES)]
        return pltpu.make_async_copy(staged[c % RING].at[tile], columns, out_sem.at[number])

    def gather(c):
        if c == final:
            finish(tail_got.at[pl.ds(1, waves - 1)], direct_recv.at[chunks])
            for pair in range(pairs):
                tail_mine[pair] = tail_got[places[pair]]
            for turn in range(1, levs):
                lev_copy(chunks, turn).start()
        finish(received[c].at[pl.ds(1, half - 1)], direct_recv.at[c])

        @pl.when(outer == 1)
        def _():
            finish(final_far[c], forward_recv.at[c])

        @pl.when(outer == 0)
        def _():
            finish(final_far[c].at[1], forward_recv.at[c])

        if c >= RING:
            for turn in range(1, levs):
                lev_copy(c - RING, turn).wait_send()
        block = ring(mine, c)

        @pl.loop(0, pairs)
        def _(pair):
            place = places[pair]
            far = place >= half
            near = received[c][lax.rem(place, half)]
            block[pair, pl.ds(0, cut)] = jnp.where(
                far, final_far[c][core, pair, pl.ds(0, cut), :], near[:cut]
            )
            block[pair, pl.ds(cut, part_rows)] = jnp.where(
                far, final_far[c][1 - core, pair], near[cut:]
            )

        for turn in range(1, levs):
            lev_copy(c, turn).start()

    def solve(c):
        for turn in range(1, levs):
            lev_copy(c, turn).wait_recv()
            if c == final:
                lev_copy(chunks, turn).wait_recv()
        if c >= RING:
            for tile in range(width_of(c - RING)):
                out_copy(c - RING, tile).wait()
        size = width_of(c) * LANES
        column = lax.broadcasted_iota(jnp.int32, (1, size), 1) + firsts[c] * LANES
        within = jnp.where(column >= width // 2, column - width // 2, column)
        own, results = ring(mine, c), staged[c % RING]

        @pl.loop(0, pairs)
        def _(pair):
            wavenumber = me * pairs + pair
            degree = jnp.where(within <= NT - wavenumber, wavenumber + within, within - 1)
            ratio = (degree * (degree + 1)).astype(jnp.float32) / float(NT * (NT + 1))
            modes = None
            for turn in range(levs):
                source = lax.rem(lev + levs - turn, levs)
                block = own[pair] if turn == 0 else theirs[c][turn - 1, pair]
                if c == final:
                    tail = tail_mine[pair] if turn == 0 else tail_theirs[turn - 1, pair]
                    block = jnp.concatenate([block, unpacked(tail)], axis=1)
                matrix = to_both.at[source]
                term = product(matrix[...], matrix[:modes_number], block, modes_number)
                modes = term if modes is None else modes + term
            scaled = modes / (1.0 + depth[...] * ratio)
            high, low = halves(scaled)
            from_high = from_both[0]
            result = jnp.dot(from_both[1], high, preferred_element_type=jnp.float32)
            result += jnp.dot(from_high, low, preferred_element_type=jnp.float32)
            result += jnp.dot(from_high, high, preferred_element_type=jnp.float32)
            for tile in range(width_of(c)):
                results[tile, pl.ds(pair, levels, stride=pairs), :] = result[
                    :, tile * LANES : (tile + 1) * LANES
                ]

        for tile in range(width_of(c)):
            out_copy(c, tile).start()

    stages = (send, relay, forward, gather, solve)
    for turn in range(chunks + LAGS[-1]):
        for stage, lag in zip(stages, LAGS):
            if 0 <= turn - lag < chunks:
                stage(turn - lag)
    finish(tail_sent, direct_send.at[chunks])
    for turn in range(1, levs):
        lev_copy(chunks, turn).wait_send()
    for c in range(max(chunks - RING, 0), chunks):
        drain_send(c)

        @pl.when(outer == 0)
        def _():
            finish(ring(relay_out, c), relay_send.at[c])
            finish(ring(forward_out, c), forward_send.at[c])

        for turn in range(1, levs):
            lev_copy(c, turn).wait_send()
        for tile in range(width_of(c)):
            out_copy(c, tile).wait()


def relay_call(waves, levs, pairs, slots, levels, width, packs, rest, room, whole, modes_number):
    parts = (1,) * whole
    chunks = len(parts)
    half = waves // 2
    part_rows = levels - levels // 2 // 8 * 8
    sizes = (waves, levs, pairs, slots, levels, width, parts, packs, rest, room)
    widths = [tiles * LANES for tiles in parts]
    most = [max(parts[c::RING]) for c in range(RING)]
    ends = [max(parts[c] + (c == chunks - 1) for c in range(k, chunks, RING)) for k in range(RING)]
    vmem, smem, anywhere = (
        pl.BlockSpec(memory_space=space) for space in (pltpu.VMEM, pltpu.SMEM, pl.ANY)
    )
    dma = pltpu.SemaphoreType.DMA
    f32, bf16 = jnp.float32, jnp.bfloat16

    def vectors(*shape):
        return pltpu.VMEM(shape, f32)

    return pl.pallas_call(
        functools.partial(relay_kernel, sizes),
        out_shape=jax.ShapeDtypeStruct((levels * pairs, (whole + 1) * LANES), f32),
        in_specs=[smem, smem, smem, smem, anywhere, anywhere, vmem, vmem, vmem],
        out_specs=anywhere,
        scratch_shapes=[vectors(half, levels, size) for size in widths]
        + [vectors(half * QUAD, part_rows, size) for size in widths]
        + [vectors(room, part_rows, size) for size in widths]
        + [vectors(2, pairs, part_rows, size) for size in widths]
        + [vectors(levs - 1, pairs, levels, size) for size in widths]
        + [vectors(tiles, levels * slots, LANES) for tiles in most]
        + [vectors(half - 1, levels, tiles * LANES) for tiles in most]
        + [vectors(QUAD, QUAD, part_rows, tiles * LANES) for tiles in most]
        + [vectors(room, part_rows, tiles * LANES) for tiles in most]
        + [vectors(3, pairs, part_rows, tiles * LANES) for tiles in most]
        + [vectors(pairs, levels, tiles * LANES) for tiles in most]
        + [vectors(tiles, levels * pairs, LANES) for tiles in ends]
        + [
            vectors(8 * packs * slots, LANES),
            vectors(waves - 1, 8, LANES),
            vectors(waves, 8, LANES),
            vectors(pairs, 8, LANES),
            vectors(levs - 1, pairs, 8, LANES),
            pltpu.VMEM((levs, 2 * modes_number, levels), bf16),
            pltpu.VMEM((2, levels, modes_number), bf16),
            dma((whole + 1,)),
            dma((chunks + 1,)),
            dma((chunks + 1,)),
            dma((chunks,)),
            dma((chunks,)),
            dma((chunks,)),
            dma((chunks,)),
            dma((chunks,)),
            dma((chunks,)),
            dma((chunks + 1, levs - 1)),
            dma((chunks + 1, levs - 1)),
            dma((whole + 1,)),
        ],
        compiler_params=pltpu.CompilerParams(
            collective_id=1, has_side_effects=True, vmem_limit_bytes=67043328
        ),
    )


def per_device(spectral, to_modes, from_modes, depth, owner):
    waves, levs = lax.axis_size("wave"), lax.axis_size("lev")
    levels, slots, width = spectral.shape
    groups = owner.shape[0] // waves
    pairs = groups * KPAIR
    modes_number = depth.shape[0]
    own_index, lev_index = lax.axis_index("wave"), lax.axis_index("lev")
    numbers = jnp.arange(owner.shape[0], dtype=jnp.int32)
    mine = owner == own_index
    before = (numbers[:, None] > numbers[None, :]) & mine[None, :]
    rank = jnp.sum(before.astype(jnp.int32), axis=1)
    picks = jnp.sum(jnp.where(mine, rank, 0).reshape(waves, groups), axis=1)
    places = lax.dynamic_slice_in_dim(owner, own_index * groups, groups) ^ own_index
    whole, rest = width // LANES, width % LANES
    packs = pl.cdiv(levels, 8)
    assert 0 < rest and packs * rest <= LANES
    parts = split(whole)
    chunks = len(parts)
    sizes = (waves, levs, pairs, slots, levels, width, parts, packs, rest)
    rows = spectral.reshape(levels * slots, width)
    last = jnp.pad(rows[:, whole * LANES :], ((0, 0), (0, LANES - rest)))
    by_lev = to_modes.reshape(modes_number, levs, levels).transpose(1, 0, 2)
    own_rows = lax.dynamic_slice_in_dim(from_modes, lev_index * levels, levels)
    vmem, smem, anywhere = (
        pl.BlockSpec(memory_space=space) for space in (pltpu.VMEM, pltpu.SMEM, pl.ANY)
    )
    dma = pltpu.SemaphoreType.DMA
    f32, bf16 = jnp.float32, jnp.bfloat16
    widths = [tiles * LANES for tiles in parts]
    staged_tiles = parts[:-1] + (parts[-1] + 1,)
    dense = pl.pallas_call(
        functools.partial(kernel, sizes),
        out_shape=jax.ShapeDtypeStruct((levels * pairs, (whole + 1) * LANES), f32),
        in_specs=[smem, smem, anywhere, anywhere, vmem, vmem, vmem],
        out_specs=anywhere,
        scratch_shapes=[pltpu.VMEM((waves, levels, size), f32) for size in widths]
        + [pltpu.VMEM((tiles, levels * slots, LANES), f32) for tiles in parts]
        + [pltpu.VMEM((waves - 1, levels, size), f32) for size in widths]
        + [pltpu.VMEM((pairs, levels, size), f32) for size in widths]
        + [pltpu.VMEM((levs - 1, pairs, levels, size), f32) for size in widths]
        + [pltpu.VMEM((tiles, levels * pairs, LANES), f32) for tiles in staged_tiles]
        + [
            pltpu.VMEM((8 * packs * slots, LANES), f32),
            pltpu.VMEM((waves - 1, 8, LANES), f32),
            pltpu.VMEM((waves, 8, LANES), f32),
            pltpu.VMEM((pairs, 8, LANES), f32),
            pltpu.VMEM((levs - 1, pairs, 8, LANES), f32),
            pltpu.VMEM((levs, 2 * modes_number, levels), bf16),
            pltpu.VMEM((2, levels, modes_number), bf16),
            dma((whole + 1,)),
            dma((chunks + 1,)),
            dma((chunks + 1,)),
            dma((chunks + 1, levs - 1)),
            dma((chunks + 1, levs - 1)),
            dma((whole + 1,)),
        ],
        compiler_params=pltpu.CompilerParams(
            collective_id=0, has_side_effects=True, vmem_limit_bytes=67043328
        ),
    )
    operands = (rows, last, by_lev, own_rows, depth[:, None])
    if waves == 4 * QUAD:
        half = waves // 2
        room = half * QUAD * 3 // 4
        owners = owner.reshape(2, 2, 2, 2, groups).transpose(0, 2, 1, 3, 4).reshape(2, 2, QUAD * groups)
        crossing = (owners // half != jnp.arange(2)[:, None, None]).astype(jnp.int32)
        inclusive = jnp.tril(jnp.ones((QUAD * groups,) * 2, jnp.int32))
        before = jnp.sum(crossing[:, :, None, :] * inclusive, axis=-1)
        fits = jnp.max(before[:, :, -1]) <= room
        side, column = own_index // half, own_index // 2 % 2
        there = before[1 - side, column] - 1
        taken = (there[None, :] == jnp.arange(room)[:, None]) & (crossing[1 - side, column] > 0)[None, :]
        target = jnp.arange(QUAD * groups, dtype=jnp.int32) // groups
        number = ((owners[1 - side, column] ^ own_index) % half) * QUAD + target
        relayed = jnp.sum(jnp.where(taken, number[None, :], 0), axis=1).astype(jnp.int32)
        here = jnp.where(crossing[side, column] > 0, before[side, column] - 1, 0).reshape(QUAD, groups)
        own_target = own_index // QUAD % 2 * 2 + own_index % 2
        landed = here[own_target ^ jnp.array([3, 2, 1, 0])].reshape(-1).astype(jnp.int32)
        solved = lax.cond(
            fits,
            lambda *given: relay_call(waves, levs, pairs, slots, levels, width, packs, rest, room, whole, modes_number)(*given),
            lambda one, two, three, four, *given: dense(one, two, *given),
            *(picks, places, relayed, landed, *operands),
        )
    else:
        solved = dense(picks, places, *operands)
    return solved.reshape(levels, pairs, (whole + 1) * LANES)[:, :, :width]


def solution(mesh):
    placed = (P("lev", "wave", None), P(), P(), P(), P())
    return jax.shard_map(
        per_device, mesh=mesh, in_specs=placed, out_specs=P("lev", "wave", None), check_vma=False
    )
```

```python
import functools

import jax
import jax.numpy as jnp
from jax import lax
from jax.experimental import pallas as pl
from jax.experimental.pallas import tpu as pltpu
from jax.sharding import PartitionSpec as P

NT = 1279
KPAIR = 1
LANES = 128
TILES = 3
HEAD = (1, 2, 2)
TAIL = (2, 2, 1, 1)
AHEAD = 2
QUAD = 4
GROUP = 4
RING = 3
LAGS = (0, 1, 2, 3, 4)
MESH = pl.DeviceIdType.MESH


def split(whole):
    middle = whole - sum(HEAD) - sum(TAIL)
    if middle < 0:
        return (1,) * whole
    rest = (middle % TILES,) if middle % TILES else ()
    return HEAD + (TILES,) * (middle // TILES) + rest + TAIL


def flipped(index, mask, count):
    result = index * 0
    bit = 1
    while bit < count:
        own = lax.rem(lax.div(index, bit), 2)
        result = result + bit * ((1 - own) if mask & bit else own)
        bit *= 2
    return result


def halves(value):
    high = value.astype(jnp.bfloat16)
    low = (value - high.astype(jnp.float32)).astype(jnp.bfloat16)
    return high, low


def upright(row):
    count = row.shape[1]
    across = lax.broadcasted_iota(jnp.int32, (count, count), 1)
    down = lax.broadcasted_iota(jnp.int32, (count, count), 0)
    return jnp.sum(jnp.where(across == down, row[...], 0.0), axis=1, keepdims=True)


def tables(waves, groups, room, owner, picks, places, relayed, landed, fits, crossed):
    half = waves // 2
    me = lax.axis_index("wave")
    side, column = lax.div(me, half), lax.rem(lax.div(me, 2), 2)
    own_target = lax.rem(lax.div(me, QUAD), 2) * 2 + lax.rem(me, 2)
    for target in range(waves):
        picks[target] = 0
    for slot in range(room):
        relayed[slot] = 0
    for pool in range(4):
        crossed[pool] = 0

    def per_target(target, rank):
        there = lax.div(target, half)
        pool = there * 2 + lax.rem(lax.div(target, 2), 2)
        j = lax.rem(lax.div(target, QUAD), 2) * 2 + lax.rem(target, 2)
        relays = pool == (1 - side) * 2 + column
        lands = pool == side * 2 + column
        number = (QUAD - 1 - (j ^ own_target)) * groups
        position = crossed[pool]
        for group in range(groups):
            source = owner[target * groups + group]
            mine = source == me
            picks[target] = jnp.where(mine, rank, picks[target])
            rank = rank + mine.astype(jnp.int32)
            crossing = lax.div(source, half) != there
            slot = jnp.minimum(position, room - 1)

            @pl.when(relays & crossing)
            def _():
                relayed[slot] = lax.rem(source ^ me, half) * QUAD + j

            @pl.when(lands)
            def _():
                landed[number + group] = jnp.where(crossing, slot, 0)

            position = position + crossing.astype(jnp.int32)
        crossed[pool] = position
        return rank

    lax.fori_loop(0, waves, per_target, jnp.int32(0))
    for group in range(groups):
        places[group] = owner[me * groups + group] ^ me
    most = jnp.maximum(
        jnp.maximum(crossed[0], crossed[1]), jnp.maximum(crossed[2], crossed[3])
    )
    fits[0] = (most <= room).astype(jnp.int32)


def product(left_both, left_high, right, rows):
    high, low = halves(right)
    both = jnp.dot(left_both, high, preferred_element_type=jnp.float32)
    cross = jnp.dot(left_high, low, preferred_element_type=jnp.float32)
    return (both[rows:] + cross) + both[:rows]


def kernel(sizes, picks, places, spectral, last, to_modes, from_modes, depth, solved, *scratch):
    waves, levs, pairs, slots, levels, width, parts, packs, rest = sizes
    chunks = len(parts)
    received, rows_in, sending, mine, theirs, staged = (
        scratch[kind * chunks : (kind + 1) * chunks] for kind in range(6)
    )
    rows_last, tail_sent, tail_got, tail_mine, tail_theirs = scratch[6 * chunks : 6 * chunks + 5]
    to_both, from_both, load_sem, send_sem, recv_sem, lev_send, lev_recv, out_sem = scratch[
        6 * chunks + 5 :
    ]
    me = lax.axis_index("wave")
    lev = lax.axis_index("lev")
    modes_number = depth.shape[1]
    firsts = [sum(parts[:c]) for c in range(chunks)]
    final = chunks - 1

    def load(c, tile):
        number = firsts[c] + tile
        if number < sum(parts):
            source = spectral.at[:, pl.ds(number * LANES, LANES)]
            return pltpu.make_async_copy(source, rows_in[c].at[tile], load_sem.at[number])
        target = rows_last.at[pl.ds(0, levels * slots)]
        return pltpu.make_async_copy(last, target, load_sem.at[number])

    def width_of(c):
        return parts[c] + (1 if c == final else 0)

    for c in range(chunks):
        for tile in range(width_of(c)):
            load(c, tile).start()

    barrier = pltpu.get_barrier_semaphore()
    for mask in range(1, waves):
        pl.semaphore_signal(
            barrier, inc=1, device_id={"wave": flipped(me, mask, waves)}, device_id_type=MESH
        )
    for turn in range(1, levs):
        pl.semaphore_signal(
            barrier, inc=1, device_id={"lev": lax.rem(lev + turn, levs)}, device_id_type=MESH
        )

    for part in range(levs):
        high, low = halves(to_modes[:, part * levels : (part + 1) * levels])
        to_both[part, :modes_number] = high
        to_both[part, modes_number:] = low
    for part in range(levs):

        @pl.when(lev == part)
        def _():
            high, low = halves(from_modes[part * levels : (part + 1) * levels, :])
            from_both[0], from_both[1] = high, low

    pl.semaphore_wait(barrier, waves + levs - 2)

    def packed(slot):
        lane = lax.broadcasted_iota(jnp.int32, (8, LANES), 1)
        total = rows_last[pl.ds(slot, 8, stride=slots), :]
        for k in range(1, packs):
            block = rows_last[pl.ds(8 * k * slots + slot, 8, stride=slots), :]
            total = jnp.where(lane >= k * rest, pltpu.roll(block, k * rest, 1), total)
        return total

    def unpacked(block):
        pieces = [block] + [pltpu.roll(block, LANES - k * rest, 1) for k in range(1, packs)]
        return jnp.concatenate(pieces, axis=0)[:levels]

    def send(c):
        for tile in range(width_of(c)):
            load(c, tile).wait()

        def pick(mask, target):
            slot = picks[flipped(me, mask, waves)]
            for tile in range(parts[c]):
                target[:, pl.ds(tile * LANES, LANES)] = rows_in[c][
                    tile, pl.ds(slot, levels, stride=slots), :
                ]

        def push(mask, source, target, number):
            pltpu.make_async_remote_copy(
                src_ref=source.at[mask - 1],
                dst_ref=target.at[mask],
                send_sem=send_sem.at[number],
                recv_sem=recv_sem.at[number],
                device_id={"wave": flipped(me, mask, waves)},
                device_id_type=MESH,
            ).start()

        if c == final:
            for mask in range(waves - 1, 0, -1):
                tail_sent[mask - 1] = packed(picks[flipped(me, mask, waves)])
                push(mask, tail_sent, tail_got, chunks)
            tail_got[0] = packed(picks[me])
        for mask in range(waves - 1, 0, -1):
            pick(mask, sending[c].at[mask - 1])
            push(mask, sending[c], received[c], c)
        pick(0, received[c].at[0])

    def lev_copy(c, turn):
        source, target = (tail_mine, tail_theirs) if c == chunks else (mine[c], theirs[c])
        return pltpu.make_async_remote_copy(
            src_ref=source,
            dst_ref=target.at[turn - 1],
            send_sem=lev_send.at[c, turn - 1],
            recv_sem=lev_recv.at[c, turn - 1],
            device_id={"lev": lax.rem(lev + turn, levs)},
            device_id_type=MESH,
        )

    def out_copy(c, tile):
        number = firsts[c] + tile
        columns = solved.at[:, pl.ds(number * LANES, LANES)]
        return pltpu.make_async_copy(staged[c].at[tile], columns, out_sem.at[number])

    def gather(c):
        if c == final:
            arrived = tail_got.at[pl.ds(1, waves - 1)]
            pltpu.make_async_copy(arrived, arrived, recv_sem.at[chunks]).wait()
            for pair in range(pairs):
                tail_mine[pair] = tail_got[places[pair]]
            for turn in range(1, levs):
                lev_copy(chunks, turn).start()
        arrived = received[c].at[pl.ds(1, waves - 1)]
        pltpu.make_async_copy(arrived, arrived, recv_sem.at[c]).wait()

        @pl.loop(0, pairs)
        def _(pair):
            mine[c][pair] = received[c][places[pair]]

        for turn in range(1, levs):
            lev_copy(c, turn).start()

    def solve(c):
        for turn in range(1, levs):
            lev_copy(c, turn).wait_recv()
            if c == final:
                lev_copy(chunks, turn).wait_recv()
        size = width_of(c) * LANES
        column = lax.broadcasted_iota(jnp.int32, (1, size), 1) + firsts[c] * LANES
        within = jnp.where(column >= width // 2, column - width // 2, column)
        column_depth = upright(depth)

        @pl.loop(0, pairs)
        def _(pair):
            wavenumber = me * pairs + pair
            degree = jnp.where(within <= NT - wavenumber, wavenumber + within, within - 1)
            ratio = (degree * (degree + 1)).astype(jnp.float32) / float(NT * (NT + 1))
            modes = None
            for turn in range(levs):
                source = lax.rem(lev + levs - turn, levs)
                block = mine[c][pair] if turn == 0 else theirs[c][turn - 1, pair]
                if c == final:
                    tail = tail_mine[pair] if turn == 0 else tail_theirs[turn - 1, pair]
                    block = jnp.concatenate([block, unpacked(tail)], axis=1)
                matrix = to_both.at[source]
                term = product(matrix[...], matrix[:modes_number], block, modes_number)
                modes = term if modes is None else modes + term
            scaled = modes / (1.0 + column_depth * ratio)
            high, low = halves(scaled)
            from_high = from_both[0]
            result = jnp.dot(from_both[1], high, preferred_element_type=jnp.float32)
            result += jnp.dot(from_high, low, preferred_element_type=jnp.float32)
            result += jnp.dot(from_high, high, preferred_element_type=jnp.float32)
            for tile in range(width_of(c)):
                staged[c][tile, pl.ds(pair, levels, stride=pairs), :] = result[
                    :, tile * LANES : (tile + 1) * LANES
                ]

        for tile in range(width_of(c)):
            out_copy(c, tile).start()

    for c in range(min(AHEAD, chunks)):
        send(c)
    for c in range(chunks):
        if c + AHEAD < chunks:
            send(c + AHEAD)
        gather(c)
        if c >= 1:
            solve(c - 1)
    solve(final)
    for c in range(chunks + 1):
        sent = tail_sent if c == chunks else sending[c]
        pltpu.make_async_copy(sent, sent, send_sem.at[c]).wait()
        for turn in range(1, levs):
            lev_copy(c, turn).wait_send()
    for c in range(chunks):
        for tile in range(width_of(c)):
            out_copy(c, tile).wait()


def relay_kernel(sizes, picks, places, relayed, landed, spectral, last, to_modes, from_modes, depth, solved, *scratch):
    waves, levs, pairs, slots, levels, width, parts, packs, rest, room = sizes
    chunks = len(parts)
    scratch = list(scratch)

    def take(count):
        taken = scratch[:count]
        del scratch[:count]
        return taken

    received, carried, arrived_far, final_far, theirs = (take(chunks) for _ in range(5))
    rows_in, direct_out, carry_out, relay_out, forward_out, mine, staged = (
        take(RING) for _ in range(7)
    )
    rows_last, tail_sent, tail_got, tail_mine, tail_theirs, to_both, from_both = take(7)
    (load_sem, direct_send, direct_recv, carry_send, carry_recv, relay_send, relay_recv,
     forward_send, forward_recv, lev_send, lev_recv, out_sem) = take(12)
    me = lax.axis_index("wave")
    lev = lax.axis_index("lev")
    half = waves // 2
    side = lax.div(me, half)
    step = lax.rem(lax.div(me, QUAD), 2)
    quad = lax.rem(me, QUAD)
    core = lax.rem(me, 2)
    outer = lax.rem(side + step + 1, 2)
    part_rows = levels // 2
    modes_number = depth.shape[1]
    firsts = [sum(parts[:c]) for c in range(chunks)]
    final = chunks - 1

    def ring(buffers, c):
        return buffers[c % RING]

    def to_wave(index):
        return {"wave": index}

    def load(c, tile):
        number = firsts[c] + tile
        if tile < parts[c]:
            source = spectral.at[:, pl.ds(number * LANES, LANES)]
            return pltpu.make_async_copy(source, rows_in[c % RING].at[tile], load_sem.at[number])
        target = rows_last.at[pl.ds(0, levels * slots)]
        return pltpu.make_async_copy(last, target, load_sem.at[number])

    def width_of(c):
        return parts[c] + (1 if c == final else 0)

    def finish(ref, semaphore):
        pltpu.make_async_copy(ref, ref, semaphore).wait()

    def push(source, target, send_sem, recv_sem, index):
        pltpu.make_async_remote_copy(
            src_ref=source,
            dst_ref=target,
            send_sem=send_sem,
            recv_sem=recv_sem,
            device_id=to_wave(index),
            device_id_type=MESH,
        ).start()

    load(final, parts[final]).start()
    for c in range(min(RING, chunks)):
        for tile in range(parts[c]):
            load(c, tile).start()

    barrier = pltpu.get_barrier_semaphore()
    for mask in range(1, waves):
        pl.semaphore_signal(
            barrier, inc=1, device_id=to_wave(flipped(me, mask, waves)), device_id_type=MESH
        )
    for turn in range(1, levs):
        pl.semaphore_signal(
            barrier, inc=1, device_id={"lev": lax.rem(lev + turn, levs)}, device_id_type=MESH
        )
    for part in range(levs):
        high, low = halves(to_modes[:, part * levels : (part + 1) * levels])
        to_both[part, :modes_number] = high
        to_both[part, modes_number:] = low
    for part in range(levs):

        @pl.when(lev == part)
        def _():
            high, low = halves(from_modes[part * levels : (part + 1) * levels, :])
            from_both[0], from_both[1] = high, low

    pl.semaphore_wait(barrier, waves + levs - 2)

    def packed(slot):
        lane = lax.broadcasted_iota(jnp.int32, (8, LANES), 1)
        total = rows_last[pl.ds(slot, 8, stride=slots), :]
        for k in range(1, packs):
            block = rows_last[pl.ds(8 * k * slots + slot, 8, stride=slots), :]
            total = jnp.where(lane >= k * rest, pltpu.roll(block, k * rest, 1), total)
        return total

    def unpacked(block):
        pieces = [block] + [pltpu.roll(block, LANES - k * rest, 1) for k in range(1, packs)]
        return jnp.concatenate(pieces, axis=0)[:levels]

    def drain_send(c):
        finish(ring(direct_out, c), direct_send.at[c])
        carry = ring(carry_out, c)

        @pl.when(outer == 1)
        def _():
            finish(carry, carry_send.at[c])

        @pl.when(outer == 0)
        def _():
            finish(carry.at[pl.ds(1, QUAD - 1)], carry_send.at[c])

    def send(c):
        for tile in range(width_of(c)):
            load(c, tile).wait()
        if c >= RING:
            drain_send(c - RING)
        source = rows_in[c % RING]
        carry, direct = ring(carry_out, c), ring(direct_out, c)

        def pick(slot, first, count):
            return source[0, pl.ds(first * slots + slot, count, stride=slots), :]

        for mask in range(QUAD - 1, -1, -1):
            carrier = flipped(quad, mask, QUAD)
            first = lax.rem(carrier, 2) * part_rows

            @pl.loop(0, QUAD)
            def _(j):
                index = (1 - side) * half + lax.div(j, 2) * QUAD
                index = index + lax.div(carrier, 2) * 2 + lax.rem(j, 2)
                carry[mask, pl.ds(j, part_rows, stride=QUAD), :] = pick(
                    picks[index], first, part_rows
                )

            place = mask + QUAD * outer
            device = side * half + (1 - side) * QUAD + carrier

            def carry_on():
                target = carried[c].at[place]
                push(carry.at[mask], target, carry_send.at[c], carry_recv.at[c], device)

            if mask:
                carry_on()
            else:
                pl.when(outer == 1)(carry_on)

                @pl.when(outer == 0)
                def _():
                    carried[c][0] = carry[0]

        if c == final:
            for mask in range(waves - 1, 0, -1):
                index = flipped(me, mask, waves)
                tail_sent[mask - 1] = packed(picks[index])
                push(
                    tail_sent.at[mask - 1],
                    tail_got.at[mask],
                    direct_send.at[chunks],
                    direct_recv.at[chunks],
                    index,
                )
            tail_got[0] = packed(picks[me])
        for mask in range(half - 1, 0, -1):
            index = flipped(me, mask, waves)
            direct[mask - 1] = pick(picks[index], 0, levels)
            push(
                direct.at[mask - 1],
                received[c].at[mask],
                direct_send.at[c],
                direct_recv.at[c],
                index,
            )
        received[c][0] = pick(picks[me], 0, levels)
        if c + RING < chunks:
            for tile in range(parts[c + RING]):
                load(c + RING, tile).start()

    def relay(c):
        @pl.when(outer == 0)
        def _():
            finish(carried[c].at[pl.ds(1, half - 1)], carry_recv.at[c])
            if c >= RING:
                finish(ring(relay_out, c - RING), relay_send.at[c - RING])
            block = ring(relay_out, c)

            @pl.loop(0, room)
            def _(g):
                number = relayed[g]
                block[pl.ds(g, part_rows, stride=room), :] = carried[c][
                    lax.div(number, QUAD), pl.ds(lax.rem(number, QUAD), part_rows, stride=QUAD), :
                ]

            push(
                block, arrived_far[c], relay_send.at[c], relay_recv.at[c],
                flipped(me, 3 * QUAD, waves),
            )

    def forward(c):
        @pl.when(outer == 0)
        def _():
            finish(arrived_far[c], relay_recv.at[c])
            if c >= RING:
                finish(ring(forward_out, c - RING), forward_send.at[c - RING])
            block = ring(forward_out, c)
            for number, mask in enumerate((QUAD + 1, QUAD, 1)):

                @pl.loop(0, pairs)
                def _(pair):
                    start = landed[number * pairs + pair]
                    block[number, pl.ds(pair, part_rows, stride=pairs), :] = arrived_far[c][
                        pl.ds(start, part_rows, stride=room), :
                    ]

                push(
                    block.at[number],
                    final_far[c].at[mask % 2],
                    forward_send.at[c],
                    forward_recv.at[c],
                    flipped(me, mask, waves),
                )

            @pl.loop(0, pairs)
            def _(pair):
                start = landed[3 * pairs + pair]
                final_far[c][0, pl.ds(pair, part_rows, stride=pairs), :] = arrived_far[c][
                    pl.ds(start, part_rows, stride=room), :
                ]

    def lev_copy(c, turn):
        source, target = (
            (tail_mine, tail_theirs) if c == chunks else (ring(mine, c), theirs[c])
        )
        return pltpu.make_async_remote_copy(
            src_ref=source,
            dst_ref=target.at[turn - 1],
            send_sem=lev_send.at[c, turn - 1],
            recv_sem=lev_recv.at[c, turn - 1],
            device_id={"lev": lax.rem(lev + turn, levs)},
            device_id_type=MESH,
        )

    def out_copy(c, tile):
        number = firsts[c] + tile
        columns = solved.at[:, pl.ds(number * LANES, LANES)]
        return pltpu.make_async_copy(staged[c % RING].at[tile], columns, out_sem.at[number])

    def gather(c):
        if c == final:
            finish(tail_got.at[pl.ds(1, waves - 1)], direct_recv.at[chunks])
            for pair in range(pairs):
                tail_mine[pair] = tail_got[places[pair]]
            for turn in range(1, levs):
                lev_copy(chunks, turn).start()
        finish(received[c].at[pl.ds(1, half - 1)], direct_recv.at[c])

        @pl.when(outer == 1)
        def _():
            finish(final_far[c], forward_recv.at[c])

        @pl.when(outer == 0)
        def _():
            finish(final_far[c].at[1], forward_recv.at[c])

        if c >= RING:
            for turn in range(1, levs):
                lev_copy(c - RING, turn).wait_send()
        block = ring(mine, c)

        @pl.loop(0, pairs)
        def _(pair):
            place = places[pair]
            far = place >= half
            near = lax.rem(place, half)
            for part, slot in enumerate((core, 1 - core)):
                first = part * part_rows
                block[pl.ds(first * pairs + pair, part_rows, stride=pairs), :] = jnp.where(
                    far,
                    final_far[c][slot, pl.ds(pair, part_rows, stride=pairs), :],
                    received[c][near, pl.ds(first, part_rows), :],
                )

        for turn in range(1, levs):
            lev_copy(c, turn).start()

    def solve(c):
        for turn in range(1, levs):
            lev_copy(c, turn).wait_recv()
            if c == final:
                lev_copy(chunks, turn).wait_recv()
        if c >= RING:
            for tile in range(width_of(c - RING)):
                out_copy(c - RING, tile).wait()
        size = width_of(c) * LANES
        column = lax.broadcasted_iota(jnp.int32, (1, size), 1) + firsts[c] * LANES
        within = jnp.where(column >= width // 2, column - width // 2, column)
        column_depth = upright(depth)
        own, results = ring(mine, c), staged[c % RING]

        @pl.loop(0, pairs // GROUP)
        def _(number):
            ratios = []
            for at in range(GROUP):
                wavenumber = me * pairs + number * GROUP + at
                degree = jnp.where(within <= NT - wavenumber, wavenumber + within, within - 1)
                ratios.append((degree * (degree + 1)).astype(jnp.float32) / float(NT * (NT + 1)))
            ratio = jnp.concatenate(ratios, axis=1)
            modes = None
            for turn in range(levs):
                source = lax.rem(lev + levs - turn, levs)
                blocks = []
                for at in range(GROUP):
                    pair = number * GROUP + at
                    rows = pl.ds(pair, levels, stride=pairs)
                    blocks.append(own[rows, :] if turn == 0 else theirs[c][turn - 1, rows, :])
                    if c == final:
                        tail = tail_mine[pair] if turn == 0 else tail_theirs[turn - 1, pair]
                        blocks.append(unpacked(tail))
                matrix = to_both.at[source]
                block = jnp.concatenate(blocks, axis=1)
                term = product(matrix[...], matrix[:modes_number], block, modes_number)
                modes = term if modes is None else modes + term
            scaled = modes / (1.0 + column_depth * ratio)
            high, low = halves(scaled)
            from_high = from_both[0]
            result = jnp.dot(from_both[1], high, preferred_element_type=jnp.float32)
            result += jnp.dot(from_high, low, preferred_element_type=jnp.float32)
            result += jnp.dot(from_high, high, preferred_element_type=jnp.float32)
            for at in range(GROUP):
                pair = number * GROUP + at
                for tile in range(width_of(c)):
                    first = at * size + tile * LANES
                    results[tile, pl.ds(pair, levels, stride=pairs), :] = result[
                        :, first : first + LANES
                    ]

        for tile in range(width_of(c)):
            out_copy(c, tile).start()

    stages = (send, relay, forward, gather, solve)
    for turn in range(chunks + LAGS[-1]):
        for stage, lag in zip(stages, LAGS):
            if 0 <= turn - lag < chunks:
                stage(turn - lag)
    finish(tail_sent, direct_send.at[chunks])
    for turn in range(1, levs):
        lev_copy(chunks, turn).wait_send()
    for c in range(max(chunks - RING, 0), chunks):
        drain_send(c)

        @pl.when(outer == 0)
        def _():
            finish(ring(relay_out, c), relay_send.at[c])
            finish(ring(forward_out, c), forward_send.at[c])

        for turn in range(1, levs):
            lev_copy(c, turn).wait_send()
        for tile in range(width_of(c)):
            out_copy(c, tile).wait()


def relay_call(waves, levs, pairs, slots, levels, width, packs, rest, room, whole, modes_number):
    parts = (1,) * whole
    chunks = len(parts)
    half = waves // 2
    part_rows = levels // 2
    sizes = (waves, levs, pairs, slots, levels, width, parts, packs, rest, room)
    vmem, smem, anywhere = (
        pl.BlockSpec(memory_space=space) for space in (pltpu.VMEM, pltpu.SMEM, pl.ANY)
    )
    dma = pltpu.SemaphoreType.DMA
    f32, bf16 = jnp.float32, jnp.bfloat16

    def vectors(*shape):
        return pltpu.VMEM(shape, f32)

    return pl.pallas_call(
        functools.partial(relay_kernel, sizes),
        out_shape=jax.ShapeDtypeStruct((levels * pairs, (whole + 1) * LANES), f32),
        in_specs=[smem, smem, smem, smem, anywhere, anywhere, vmem, vmem, vmem],
        out_specs=anywhere,
        scratch_shapes=[vectors(half, levels, LANES)] * chunks
        + [vectors(half, QUAD * part_rows, LANES)] * chunks
        + [vectors(room * part_rows, LANES)] * chunks
        + [vectors(2, pairs * part_rows, LANES)] * chunks
        + [vectors(levs - 1, pairs * levels, LANES)] * chunks
        + [vectors(1, levels * slots, LANES)] * RING
        + [vectors(half - 1, levels, LANES)] * RING
        + [vectors(QUAD, QUAD * part_rows, LANES)] * RING
        + [vectors(room * part_rows, LANES)] * RING
        + [vectors(3, pairs * part_rows, LANES)] * RING
        + [vectors(pairs * levels, LANES)] * RING
        + [vectors(2, levels * pairs, LANES)] * RING
        + [
            vectors(8 * packs * slots, LANES),
            vectors(waves - 1, 8, LANES),
            vectors(waves, 8, LANES),
            vectors(pairs, 8, LANES),
            vectors(levs - 1, pairs, 8, LANES),
            pltpu.VMEM((levs, 2 * modes_number, levels), bf16),
            pltpu.VMEM((2, levels, modes_number), bf16),
            dma((whole + 1,)),
            dma((chunks + 1,)),
            dma((chunks + 1,)),
            dma((chunks,)),
            dma((chunks,)),
            dma((chunks,)),
            dma((chunks,)),
            dma((chunks,)),
            dma((chunks,)),
            dma((chunks + 1, levs - 1)),
            dma((chunks + 1, levs - 1)),
            dma((whole + 1,)),
        ],
        compiler_params=pltpu.CompilerParams(
            collective_id=1, has_side_effects=True, vmem_limit_bytes=67043328
        ),
    )


def per_device(spectral, to_modes, from_modes, depth, owner):
    waves, levs = lax.axis_size("wave"), lax.axis_size("lev")
    levels, slots, width = spectral.shape
    groups = owner.shape[0] // waves
    pairs = groups * KPAIR
    modes_number = depth.shape[0]
    own_index = lax.axis_index("wave")
    whole, rest = width // LANES, width % LANES
    packs = pl.cdiv(levels, 8)
    assert 0 < rest and packs * rest <= LANES
    parts = split(whole)
    chunks = len(parts)
    sizes = (waves, levs, pairs, slots, levels, width, parts, packs, rest)
    rows = spectral.reshape(levels * slots, width)
    last = jnp.pad(rows[:, whole * LANES :], ((0, 0), (0, LANES - rest)))
    vmem, smem, anywhere = (
        pl.BlockSpec(memory_space=space) for space in (pltpu.VMEM, pltpu.SMEM, pl.ANY)
    )
    dma = pltpu.SemaphoreType.DMA
    f32, bf16 = jnp.float32, jnp.bfloat16
    widths = [tiles * LANES for tiles in parts]
    staged_tiles = parts[:-1] + (parts[-1] + 1,)
    dense = pl.pallas_call(
        functools.partial(kernel, sizes),
        out_shape=jax.ShapeDtypeStruct((levels * pairs, (whole + 1) * LANES), f32),
        in_specs=[smem, smem, anywhere, anywhere, vmem, vmem, vmem],
        out_specs=anywhere,
        scratch_shapes=[pltpu.VMEM((waves, levels, size), f32) for size in widths]
        + [pltpu.VMEM((tiles, levels * slots, LANES), f32) for tiles in parts]
        + [pltpu.VMEM((waves - 1, levels, size), f32) for size in widths]
        + [pltpu.VMEM((pairs, levels, size), f32) for size in widths]
        + [pltpu.VMEM((levs - 1, pairs, levels, size), f32) for size in widths]
        + [pltpu.VMEM((tiles, levels * pairs, LANES), f32) for tiles in staged_tiles]
        + [
            pltpu.VMEM((8 * packs * slots, LANES), f32),
            pltpu.VMEM((waves - 1, 8, LANES), f32),
            pltpu.VMEM((waves, 8, LANES), f32),
            pltpu.VMEM((pairs, 8, LANES), f32),
            pltpu.VMEM((levs - 1, pairs, 8, LANES), f32),
            pltpu.VMEM((levs, 2 * modes_number, levels), bf16),
            pltpu.VMEM((2, levels, modes_number), bf16),
            dma((whole + 1,)),
            dma((chunks + 1,)),
            dma((chunks + 1,)),
            dma((chunks + 1, levs - 1)),
            dma((chunks + 1, levs - 1)),
            dma((whole + 1,)),
        ],
        compiler_params=pltpu.CompilerParams(
            collective_id=0, has_side_effects=True, vmem_limit_bytes=67043328
        ),
    )
    operands = (rows, last, to_modes, from_modes, depth[None, :])
    if waves == 4 * QUAD and levels % 2 == 0:
        half = waves // 2
        room = half * QUAD * 3 // 4
        int_shapes = [waves, groups, room, QUAD * groups, 1]
        picks, places, relayed, landed, fits = pl.pallas_call(
            functools.partial(tables, waves, groups, room),
            out_shape=[jax.ShapeDtypeStruct((size,), jnp.int32) for size in int_shapes],
            in_specs=[smem],
            out_specs=[smem] * 5,
            scratch_shapes=[pltpu.SMEM((4,), jnp.int32)],
        )(owner)
        solved = lax.cond(
            fits[0] > 0,
            lambda *given: relay_call(waves, levs, pairs, slots, levels, width, packs, rest, room, whole, modes_number)(*given),
            lambda one, two, three, four, *given: dense(one, two, *given),
            *(picks, places, relayed, landed, *operands),
        )
    else:
        numbers = jnp.arange(owner.shape[0], dtype=jnp.int32)
        mine = owner == own_index
        before = (numbers[:, None] > numbers[None, :]) & mine[None, :]
        rank = jnp.sum(before.astype(jnp.int32), axis=1)
        picks = jnp.sum(jnp.where(mine, rank, 0).reshape(waves, groups), axis=1)
        places = lax.dynamic_slice_in_dim(owner, own_index * groups, groups) ^ own_index
        solved = dense(picks, places, *operands)
    return solved.reshape(levels, pairs, (whole + 1) * LANES)[:, :, :width]


def solution(mesh):
    placed = (P("lev", "wave", None), P(), P(), P(), P())
    return jax.shard_map(
        per_device, mesh=mesh, in_specs=placed, out_specs=P("lev", "wave", None), check_vma=False
    )
```

```python
import functools

import jax
import jax.numpy as jnp
from jax import lax
from jax.experimental import pallas as pl
from jax.experimental.pallas import tpu as pltpu
from jax.sharding import PartitionSpec as P

NT = 1279
KPAIR = 1
LANES = 128
TILES = 3
HEAD = (1, 2, 2)
TAIL = (2, 2, 1, 1)
AHEAD = 2
QUAD = 4
GROUP = 4
RING = 3
LAGS = (0, 1, 1, 2, 3, 4)
MESH = pl.DeviceIdType.MESH


def split(whole):
    middle = whole - sum(HEAD) - sum(TAIL)
    if middle < 0:
        return (1,) * whole
    rest = (middle % TILES,) if middle % TILES else ()
    return HEAD + (TILES,) * (middle // TILES) + rest + TAIL


def flipped(index, mask, count):
    result = index * 0
    bit = 1
    while bit < count:
        own = lax.rem(lax.div(index, bit), 2)
        result = result + bit * ((1 - own) if mask & bit else own)
        bit *= 2
    return result


def halves(value):
    high = value.astype(jnp.bfloat16)
    low = (value - high.astype(jnp.float32)).astype(jnp.bfloat16)
    return high, low


def upright(row):
    count = row.shape[1]
    across = lax.broadcasted_iota(jnp.int32, (count, count), 1)
    down = lax.broadcasted_iota(jnp.int32, (count, count), 0)
    return jnp.sum(jnp.where(across == down, row[...], 0.0), axis=1, keepdims=True)


def tables(waves, groups, room, owner, picks, places, relayed, landed, fits, crossed):
    half = waves // 2
    me = lax.axis_index("wave")
    side, column = lax.div(me, half), lax.rem(lax.div(me, 2), 2)
    own_target = lax.rem(lax.div(me, QUAD), 2) * 2 + lax.rem(me, 2)
    for target in range(waves):
        picks[target] = 0
    for slot in range(room):
        relayed[slot] = 0
    for pool in range(4):
        crossed[pool] = 0

    def per_target(target, rank):
        there = lax.div(target, half)
        pool = there * 2 + lax.rem(lax.div(target, 2), 2)
        j = lax.rem(lax.div(target, QUAD), 2) * 2 + lax.rem(target, 2)
        relays = pool == (1 - side) * 2 + column
        lands = pool == side * 2 + column
        number = (QUAD - 1 - (j ^ own_target)) * groups
        position = crossed[pool]
        for group in range(groups):
            source = owner[target * groups + group]
            mine = source == me
            picks[target] = jnp.where(mine, rank, picks[target])
            rank = rank + mine.astype(jnp.int32)
            crossing = lax.div(source, half) != there
            slot = jnp.minimum(position, room - 1)

            @pl.when(relays & crossing)
            def _():
                relayed[slot] = lax.rem(source ^ me, half) * QUAD + j

            @pl.when(lands)
            def _():
                landed[number + group] = jnp.where(crossing, slot, 0)

            position = position + crossing.astype(jnp.int32)
        crossed[pool] = position
        return rank

    lax.fori_loop(0, waves, per_target, jnp.int32(0))
    for group in range(groups):
        places[group] = owner[me * groups + group] ^ me
    most = jnp.maximum(
        jnp.maximum(crossed[0], crossed[1]), jnp.maximum(crossed[2], crossed[3])
    )
    fits[0] = (most <= room).astype(jnp.int32)


def product(left_both, left_high, right, rows):
    high, low = halves(right)
    both = jnp.dot(left_both, high, preferred_element_type=jnp.float32)
    cross = jnp.dot(left_high, low, preferred_element_type=jnp.float32)
    return (both[rows:] + cross) + both[:rows]


def kernel(sizes, picks, places, spectral, last, to_modes, from_modes, depth, solved, *scratch):
    waves, levs, pairs, slots, levels, width, parts, packs, rest = sizes
    chunks = len(parts)
    received, rows_in, sending, mine, theirs, staged = (
        scratch[kind * chunks : (kind + 1) * chunks] for kind in range(6)
    )
    rows_last, tail_sent, tail_got, tail_mine, tail_theirs = scratch[6 * chunks : 6 * chunks + 5]
    to_both, from_both, load_sem, send_sem, recv_sem, lev_send, lev_recv, out_sem = scratch[
        6 * chunks + 5 :
    ]
    me = lax.axis_index("wave")
    lev = lax.axis_index("lev")
    modes_number = depth.shape[1]
    firsts = [sum(parts[:c]) for c in range(chunks)]
    final = chunks - 1

    def load(c, tile):
        number = firsts[c] + tile
        if number < sum(parts):
            source = spectral.at[:, pl.ds(number * LANES, LANES)]
            return pltpu.make_async_copy(source, rows_in[c].at[tile], load_sem.at[number])
        target = rows_last.at[pl.ds(0, levels * slots)]
        return pltpu.make_async_copy(last, target, load_sem.at[number])

    def width_of(c):
        return parts[c] + (1 if c == final else 0)

    for c in range(chunks):
        for tile in range(width_of(c)):
            load(c, tile).start()

    barrier = pltpu.get_barrier_semaphore()
    for mask in range(1, waves):
        pl.semaphore_signal(
            barrier, inc=1, device_id={"wave": flipped(me, mask, waves)}, device_id_type=MESH
        )
    for turn in range(1, levs):
        pl.semaphore_signal(
            barrier, inc=1, device_id={"lev": lax.rem(lev + turn, levs)}, device_id_type=MESH
        )

    for part in range(levs):
        high, low = halves(to_modes[:, part * levels : (part + 1) * levels])
        to_both[part, :modes_number] = high
        to_both[part, modes_number:] = low
    for part in range(levs):

        @pl.when(lev == part)
        def _():
            high, low = halves(from_modes[part * levels : (part + 1) * levels, :])
            from_both[0], from_both[1] = high, low

    pl.semaphore_wait(barrier, waves + levs - 2)

    def packed(slot):
        lane = lax.broadcasted_iota(jnp.int32, (8, LANES), 1)
        total = rows_last[pl.ds(slot, 8, stride=slots), :]
        for k in range(1, packs):
            block = rows_last[pl.ds(8 * k * slots + slot, 8, stride=slots), :]
            total = jnp.where(lane >= k * rest, pltpu.roll(block, k * rest, 1), total)
        return total

    def unpacked(block):
        pieces = [block] + [pltpu.roll(block, LANES - k * rest, 1) for k in range(1, packs)]
        return jnp.concatenate(pieces, axis=0)[:levels]

    def send(c):
        for tile in range(width_of(c)):
            load(c, tile).wait()

        def pick(mask, target):
            slot = picks[flipped(me, mask, waves)]
            for tile in range(parts[c]):
                target[:, pl.ds(tile * LANES, LANES)] = rows_in[c][
                    tile, pl.ds(slot, levels, stride=slots), :
                ]

        def push(mask, source, target, number):
            pltpu.make_async_remote_copy(
                src_ref=source.at[mask - 1],
                dst_ref=target.at[mask],
                send_sem=send_sem.at[number],
                recv_sem=recv_sem.at[number],
                device_id={"wave": flipped(me, mask, waves)},
                device_id_type=MESH,
            ).start()

        if c == final:
            for mask in range(waves - 1, 0, -1):
                tail_sent[mask - 1] = packed(picks[flipped(me, mask, waves)])
                push(mask, tail_sent, tail_got, chunks)
            tail_got[0] = packed(picks[me])
        for mask in range(waves - 1, 0, -1):
            pick(mask, sending[c].at[mask - 1])
            push(mask, sending[c], received[c], c)
        pick(0, received[c].at[0])

    def lev_copy(c, turn):
        source, target = (tail_mine, tail_theirs) if c == chunks else (mine[c], theirs[c])
        return pltpu.make_async_remote_copy(
            src_ref=source,
            dst_ref=target.at[turn - 1],
            send_sem=lev_send.at[c, turn - 1],
            recv_sem=lev_recv.at[c, turn - 1],
            device_id={"lev": lax.rem(lev + turn, levs)},
            device_id_type=MESH,
        )

    def out_copy(c, tile):
        number = firsts[c] + tile
        columns = solved.at[:, pl.ds(number * LANES, LANES)]
        return pltpu.make_async_copy(staged[c].at[tile], columns, out_sem.at[number])

    def gather(c):
        if c == final:
            arrived = tail_got.at[pl.ds(1, waves - 1)]
            pltpu.make_async_copy(arrived, arrived, recv_sem.at[chunks]).wait()
            for pair in range(pairs):
                tail_mine[pair] = tail_got[places[pair]]
            for turn in range(1, levs):
                lev_copy(chunks, turn).start()
        arrived = received[c].at[pl.ds(1, waves - 1)]
        pltpu.make_async_copy(arrived, arrived, recv_sem.at[c]).wait()

        @pl.loop(0, pairs)
        def _(pair):
            mine[c][pair] = received[c][places[pair]]

        for turn in range(1, levs):
            lev_copy(c, turn).start()

    def solve(c):
        for turn in range(1, levs):
            lev_copy(c, turn).wait_recv()
            if c == final:
                lev_copy(chunks, turn).wait_recv()
        size = width_of(c) * LANES
        column = lax.broadcasted_iota(jnp.int32, (1, size), 1) + firsts[c] * LANES
        within = jnp.where(column >= width // 2, column - width // 2, column)
        column_depth = upright(depth)

        @pl.loop(0, pairs)
        def _(pair):
            wavenumber = me * pairs + pair
            degree = jnp.where(within <= NT - wavenumber, wavenumber + within, within - 1)
            ratio = (degree * (degree + 1)).astype(jnp.float32) / float(NT * (NT + 1))
            modes = None
            for turn in range(levs):
                source = lax.rem(lev + levs - turn, levs)
                block = mine[c][pair] if turn == 0 else theirs[c][turn - 1, pair]
                if c == final:
                    tail = tail_mine[pair] if turn == 0 else tail_theirs[turn - 1, pair]
                    block = jnp.concatenate([block, unpacked(tail)], axis=1)
                matrix = to_both.at[source]
                term = product(matrix[...], matrix[:modes_number], block, modes_number)
                modes = term if modes is None else modes + term
            scaled = modes / (1.0 + column_depth * ratio)
            high, low = halves(scaled)
            from_high = from_both[0]
            result = jnp.dot(from_both[1], high, preferred_element_type=jnp.float32)
            result += jnp.dot(from_high, low, preferred_element_type=jnp.float32)
            result += jnp.dot(from_high, high, preferred_element_type=jnp.float32)
            for tile in range(width_of(c)):
                staged[c][tile, pl.ds(pair, levels, stride=pairs), :] = result[
                    :, tile * LANES : (tile + 1) * LANES
                ]

        for tile in range(width_of(c)):
            out_copy(c, tile).start()

    for c in range(min(AHEAD, chunks)):
        send(c)
    for c in range(chunks):
        if c + AHEAD < chunks:
            send(c + AHEAD)
        gather(c)
        if c >= 1:
            solve(c - 1)
    solve(final)
    for c in range(chunks + 1):
        sent = tail_sent if c == chunks else sending[c]
        pltpu.make_async_copy(sent, sent, send_sem.at[c]).wait()
        for turn in range(1, levs):
            lev_copy(c, turn).wait_send()
    for c in range(chunks):
        for tile in range(width_of(c)):
            out_copy(c, tile).wait()


def relay_kernel(sizes, picks, places, relayed, landed, spectral, last, to_modes, from_modes, depth, solved, *scratch):
    waves, levs, pairs, slots, levels, width, parts, packs, rest, room = sizes
    chunks = len(parts)
    scratch = list(scratch)

    def take(count):
        taken = scratch[:count]
        del scratch[:count]
        return taken

    received, carried, arrived_far, final_far, theirs = (take(chunks) for _ in range(5))
    rows_in, direct_out, carry_out, relay_out, forward_out, mine, staged = (
        take(RING) for _ in range(7)
    )
    rows_last, tail_sent, tail_got, tail_mine, tail_theirs, to_both, from_both = take(7)
    (load_sem, direct_send, direct_recv, carry_send, carry_recv, relay_send, relay_recv,
     forward_send, forward_recv, lev_send, lev_recv, out_sem) = take(12)
    me = lax.axis_index("wave")
    lev = lax.axis_index("lev")
    half = waves // 2
    side = lax.div(me, half)
    step = lax.rem(lax.div(me, QUAD), 2)
    quad = lax.rem(me, QUAD)
    core = lax.rem(me, 2)
    outer = lax.rem(side + step + 1, 2)
    part_rows = levels // 2
    modes_number = depth.shape[1]
    firsts = [sum(parts[:c]) for c in range(chunks)]
    final = chunks - 1

    def ring(buffers, c):
        return buffers[c % RING]

    def to_wave(index):
        return {"wave": index}

    def load(c, tile):
        number = firsts[c] + tile
        if tile < parts[c]:
            source = spectral.at[:, pl.ds(number * LANES, LANES)]
            return pltpu.make_async_copy(source, rows_in[c % RING].at[tile], load_sem.at[number])
        target = rows_last.at[pl.ds(0, levels * slots)]
        return pltpu.make_async_copy(last, target, load_sem.at[number])

    def width_of(c):
        return parts[c] + (1 if c == final else 0)

    def finish(ref, semaphore):
        pltpu.make_async_copy(ref, ref, semaphore).wait()

    def push(source, target, send_sem, recv_sem, index):
        pltpu.make_async_remote_copy(
            src_ref=source,
            dst_ref=target,
            send_sem=send_sem,
            recv_sem=recv_sem,
            device_id=to_wave(index),
            device_id_type=MESH,
        ).start()

    load(final, parts[final]).start()
    for c in range(min(RING, chunks)):
        for tile in range(parts[c]):
            load(c, tile).start()

    barrier = pltpu.get_barrier_semaphore()
    for mask in range(1, waves):
        pl.semaphore_signal(
            barrier, inc=1, device_id=to_wave(flipped(me, mask, waves)), device_id_type=MESH
        )
    for turn in range(1, levs):
        pl.semaphore_signal(
            barrier, inc=1, device_id={"lev": lax.rem(lev + turn, levs)}, device_id_type=MESH
        )
    for part in range(levs):
        high, low = halves(to_modes[:, part * levels : (part + 1) * levels])
        to_both[part, :modes_number] = high
        to_both[part, modes_number:] = low
    for part in range(levs):

        @pl.when(lev == part)
        def _():
            high, low = halves(from_modes[part * levels : (part + 1) * levels, :])
            from_both[0], from_both[1] = high, low

    pl.semaphore_wait(barrier, waves + levs - 2)

    def packed(slot):
        lane = lax.broadcasted_iota(jnp.int32, (8, LANES), 1)
        total = rows_last[pl.ds(slot, 8, stride=slots), :]
        for k in range(1, packs):
            block = rows_last[pl.ds(8 * k * slots + slot, 8, stride=slots), :]
            total = jnp.where(lane >= k * rest, pltpu.roll(block, k * rest, 1), total)
        return total

    def unpacked(block):
        pieces = [block] + [pltpu.roll(block, LANES - k * rest, 1) for k in range(1, packs)]
        return jnp.concatenate(pieces, axis=0)[:levels]

    def pick(c, slot, first, count):
        return rows_in[c % RING][0, pl.ds(first * slots + slot, count, stride=slots), :]

    def drain_send(c):
        carry = ring(carry_out, c)

        @pl.when(outer == 1)
        def _():
            finish(carry, carry_send.at[c])

        @pl.when(outer == 0)
        def _():
            finish(carry.at[pl.ds(1, QUAD - 1)], carry_send.at[c])

    def send(c):
        for tile in range(width_of(c)):
            load(c, tile).wait()
        if c >= RING:
            drain_send(c - RING)
        carry = ring(carry_out, c)

        for mask in range(QUAD - 1, -1, -1):
            carrier = flipped(quad, mask, QUAD)
            first = lax.rem(carrier, 2) * part_rows

            @pl.loop(0, QUAD)
            def _(j):
                index = (1 - side) * half + lax.div(j, 2) * QUAD
                index = index + lax.div(carrier, 2) * 2 + lax.rem(j, 2)
                carry[mask, pl.ds(j, part_rows, stride=QUAD), :] = pick(
                    c, picks[index], first, part_rows
                )

            place = mask + QUAD * outer
            device = side * half + (1 - side) * QUAD + carrier

            def carry_on():
                target = carried[c].at[place]
                push(carry.at[mask], target, carry_send.at[c], carry_recv.at[c], device)

            if mask:
                carry_on()
            else:
                pl.when(outer == 1)(carry_on)

                @pl.when(outer == 0)
                def _():
                    carried[c][0] = carry[0]

    def near(c):
        if c >= RING:
            finish(ring(direct_out, c - RING), direct_send.at[c - RING])
        direct = ring(direct_out, c)
        if c == final:
            for mask in range(waves - 1, 0, -1):
                index = flipped(me, mask, waves)
                tail_sent[mask - 1] = packed(picks[index])
                push(
                    tail_sent.at[mask - 1],
                    tail_got.at[mask],
                    direct_send.at[chunks],
                    direct_recv.at[chunks],
                    index,
                )
            tail_got[0] = packed(picks[me])
        for mask in range(half - 1, 0, -1):
            index = flipped(me, mask, waves)
            direct[mask - 1] = pick(c, picks[index], 0, levels)
            push(
                direct.at[mask - 1],
                received[c].at[mask],
                direct_send.at[c],
                direct_recv.at[c],
                index,
            )
        received[c][0] = pick(c, picks[me], 0, levels)
        if c + RING < chunks:
            for tile in range(parts[c + RING]):
                load(c + RING, tile).start()

    def relay(c):
        @pl.when(outer == 0)
        def _():
            finish(carried[c].at[pl.ds(1, half - 1)], carry_recv.at[c])
            if c >= RING:
                finish(ring(relay_out, c - RING), relay_send.at[c - RING])
            block = ring(relay_out, c)

            @pl.loop(0, room)
            def _(g):
                number = relayed[g]
                block[pl.ds(g, part_rows, stride=room), :] = carried[c][
                    lax.div(number, QUAD), pl.ds(lax.rem(number, QUAD), part_rows, stride=QUAD), :
                ]

            push(
                block, arrived_far[c], relay_send.at[c], relay_recv.at[c],
                flipped(me, 3 * QUAD, waves),
            )

    def forward(c):
        @pl.when(outer == 0)
        def _():
            finish(arrived_far[c], relay_recv.at[c])
            if c >= RING:
                finish(ring(forward_out, c - RING), forward_send.at[c - RING])
            block = ring(forward_out, c)
            for number, mask in enumerate((QUAD + 1, QUAD, 1)):

                @pl.loop(0, pairs)
                def _(pair):
                    start = landed[number * pairs + pair]
                    block[number, pl.ds(pair, part_rows, stride=pairs), :] = arrived_far[c][
                        pl.ds(start, part_rows, stride=room), :
                    ]

                push(
                    block.at[number],
                    final_far[c].at[mask % 2],
                    forward_send.at[c],
                    forward_recv.at[c],
                    flipped(me, mask, waves),
                )

            @pl.loop(0, pairs)
            def _(pair):
                start = landed[3 * pairs + pair]
                final_far[c][0, pl.ds(pair, part_rows, stride=pairs), :] = arrived_far[c][
                    pl.ds(start, part_rows, stride=room), :
                ]

    def lev_copy(c, turn):
        source, target = (
            (tail_mine, tail_theirs) if c == chunks else (ring(mine, c), theirs[c])
        )
        return pltpu.make_async_remote_copy(
            src_ref=source,
            dst_ref=target.at[turn - 1],
            send_sem=lev_send.at[c, turn - 1],
            recv_sem=lev_recv.at[c, turn - 1],
            device_id={"lev": lax.rem(lev + turn, levs)},
            device_id_type=MESH,
        )

    def out_copy(c, tile):
        number = firsts[c] + tile
        columns = solved.at[:, pl.ds(number * LANES, LANES)]
        return pltpu.make_async_copy(staged[c % RING].at[tile], columns, out_sem.at[number])

    def gather(c):
        if c == final:
            finish(tail_got.at[pl.ds(1, waves - 1)], direct_recv.at[chunks])
            for pair in range(pairs):
                tail_mine[pair] = tail_got[places[pair]]
            for turn in range(1, levs):
                lev_copy(chunks, turn).start()
        finish(received[c].at[pl.ds(1, half - 1)], direct_recv.at[c])

        @pl.when(outer == 1)
        def _():
            finish(final_far[c], forward_recv.at[c])

        @pl.when(outer == 0)
        def _():
            finish(final_far[c].at[1], forward_recv.at[c])

        if c >= RING:
            for turn in range(1, levs):
                lev_copy(c - RING, turn).wait_send()
        block = ring(mine, c)

        @pl.loop(0, pairs)
        def _(pair):
            place = places[pair]
            far = place >= half
            near = lax.rem(place, half)
            for part, slot in enumerate((core, 1 - core)):
                first = part * part_rows
                block[pl.ds(first * pairs + pair, part_rows, stride=pairs), :] = jnp.where(
                    far,
                    final_far[c][slot, pl.ds(pair, part_rows, stride=pairs), :],
                    received[c][near, pl.ds(first, part_rows), :],
                )

        for turn in range(1, levs):
            lev_copy(c, turn).start()

    def solve(c):
        for turn in range(1, levs):
            lev_copy(c, turn).wait_recv()
            if c == final:
                lev_copy(chunks, turn).wait_recv()
        if c >= RING:
            for tile in range(width_of(c - RING)):
                out_copy(c - RING, tile).wait()
        size = width_of(c) * LANES
        column = lax.broadcasted_iota(jnp.int32, (1, size), 1) + firsts[c] * LANES
        within = jnp.where(column >= width // 2, column - width // 2, column)
        column_depth = upright(depth)
        own, results = ring(mine, c), staged[c % RING]

        @pl.loop(0, pairs // GROUP)
        def _(number):
            ratios = []
            for at in range(GROUP):
                wavenumber = me * pairs + number * GROUP + at
                degree = jnp.where(within <= NT - wavenumber, wavenumber + within, within - 1)
                ratios.append((degree * (degree + 1)).astype(jnp.float32) / float(NT * (NT + 1)))
            ratio = jnp.concatenate(ratios, axis=1)
            modes = None
            for turn in range(levs):
                source = lax.rem(lev + levs - turn, levs)
                blocks = []
                for at in range(GROUP):
                    pair = number * GROUP + at
                    rows = pl.ds(pair, levels, stride=pairs)
                    blocks.append(own[rows, :] if turn == 0 else theirs[c][turn - 1, rows, :])
                    if c == final:
                        tail = tail_mine[pair] if turn == 0 else tail_theirs[turn - 1, pair]
                        blocks.append(unpacked(tail))
                matrix = to_both.at[source]
                block = jnp.concatenate(blocks, axis=1)
                term = product(matrix[...], matrix[:modes_number], block, modes_number)
                modes = term if modes is None else modes + term
            scaled = modes / (1.0 + column_depth * ratio)
            high, low = halves(scaled)
            from_high = from_both[0]
            result = jnp.dot(from_both[1], high, preferred_element_type=jnp.float32)
            result += jnp.dot(from_high, low, preferred_element_type=jnp.float32)
            result += jnp.dot(from_high, high, preferred_element_type=jnp.float32)
            for at in range(GROUP):
                pair = number * GROUP + at
                for tile in range(width_of(c)):
                    first = at * size + tile * LANES
                    results[tile, pl.ds(pair, levels, stride=pairs), :] = result[
                        :, first : first + LANES
                    ]

        for tile in range(width_of(c)):
            out_copy(c, tile).start()

    stages = (send, relay, near, forward, gather, solve)
    for turn in range(chunks + LAGS[-1]):
        for stage, lag in zip(stages, LAGS):
            if 0 <= turn - lag < chunks:
                stage(turn - lag)
    finish(tail_sent, direct_send.at[chunks])
    for turn in range(1, levs):
        lev_copy(chunks, turn).wait_send()
    for c in range(max(chunks - RING, 0), chunks):
        drain_send(c)
        finish(ring(direct_out, c), direct_send.at[c])

        @pl.when(outer == 0)
        def _():
            finish(ring(relay_out, c), relay_send.at[c])
            finish(ring(forward_out, c), forward_send.at[c])

        for turn in range(1, levs):
            lev_copy(c, turn).wait_send()
        for tile in range(width_of(c)):
            out_copy(c, tile).wait()


def relay_call(waves, levs, pairs, slots, levels, width, packs, rest, room, whole, modes_number):
    parts = (1,) * whole
    chunks = len(parts)
    half = waves // 2
    part_rows = levels // 2
    sizes = (waves, levs, pairs, slots, levels, width, parts, packs, rest, room)
    vmem, smem, anywhere = (
        pl.BlockSpec(memory_space=space) for space in (pltpu.VMEM, pltpu.SMEM, pl.ANY)
    )
    dma = pltpu.SemaphoreType.DMA
    f32, bf16 = jnp.float32, jnp.bfloat16

    def vectors(*shape):
        return pltpu.VMEM(shape, f32)

    return pl.pallas_call(
        functools.partial(relay_kernel, sizes),
        out_shape=jax.ShapeDtypeStruct((levels * pairs, (whole + 1) * LANES), f32),
        in_specs=[smem, smem, smem, smem, anywhere, anywhere, vmem, vmem, vmem],
        out_specs=anywhere,
        scratch_shapes=[vectors(half, levels, LANES)] * chunks
        + [vectors(half, QUAD * part_rows, LANES)] * chunks
        + [vectors(room * part_rows, LANES)] * chunks
        + [vectors(2, pairs * part_rows, LANES)] * chunks
        + [vectors(levs - 1, pairs * levels, LANES)] * chunks
        + [vectors(1, levels * slots, LANES)] * RING
        + [vectors(half - 1, levels, LANES)] * RING
        + [vectors(QUAD, QUAD * part_rows, LANES)] * RING
        + [vectors(room * part_rows, LANES)] * RING
        + [vectors(3, pairs * part_rows, LANES)] * RING
        + [vectors(pairs * levels, LANES)] * RING
        + [vectors(2, levels * pairs, LANES)] * RING
        + [
            vectors(8 * packs * slots, LANES),
            vectors(waves - 1, 8, LANES),
            vectors(waves, 8, LANES),
            vectors(pairs, 8, LANES),
            vectors(levs - 1, pairs, 8, LANES),
            pltpu.VMEM((levs, 2 * modes_number, levels), bf16),
            pltpu.VMEM((2, levels, modes_number), bf16),
            dma((whole + 1,)),
            dma((chunks + 1,)),
            dma((chunks + 1,)),
            dma((chunks,)),
            dma((chunks,)),
            dma((chunks,)),
            dma((chunks,)),
            dma((chunks,)),
            dma((chunks,)),
            dma((chunks + 1, levs - 1)),
            dma((chunks + 1, levs - 1)),
            dma((whole + 1,)),
        ],
        compiler_params=pltpu.CompilerParams(
            collective_id=1, has_side_effects=True, vmem_limit_bytes=67043328
        ),
    )


def per_device(spectral, to_modes, from_modes, depth, owner):
    waves, levs = lax.axis_size("wave"), lax.axis_size("lev")
    levels, slots, width = spectral.shape
    groups = owner.shape[0] // waves
    pairs = groups * KPAIR
    modes_number = depth.shape[0]
    own_index = lax.axis_index("wave")
    whole, rest = width // LANES, width % LANES
    packs = pl.cdiv(levels, 8)
    assert 0 < rest and packs * rest <= LANES
    parts = split(whole)
    chunks = len(parts)
    sizes = (waves, levs, pairs, slots, levels, width, parts, packs, rest)
    rows = spectral.reshape(levels * slots, width)
    last = jnp.pad(rows[:, whole * LANES :], ((0, 0), (0, LANES - rest)))
    vmem, smem, anywhere = (
        pl.BlockSpec(memory_space=space) for space in (pltpu.VMEM, pltpu.SMEM, pl.ANY)
    )
    dma = pltpu.SemaphoreType.DMA
    f32, bf16 = jnp.float32, jnp.bfloat16
    widths = [tiles * LANES for tiles in parts]
    staged_tiles = parts[:-1] + (parts[-1] + 1,)
    dense = pl.pallas_call(
        functools.partial(kernel, sizes),
        out_shape=jax.ShapeDtypeStruct((levels * pairs, (whole + 1) * LANES), f32),
        in_specs=[smem, smem, anywhere, anywhere, vmem, vmem, vmem],
        out_specs=anywhere,
        scratch_shapes=[pltpu.VMEM((waves, levels, size), f32) for size in widths]
        + [pltpu.VMEM((tiles, levels * slots, LANES), f32) for tiles in parts]
        + [pltpu.VMEM((waves - 1, levels, size), f32) for size in widths]
        + [pltpu.VMEM((pairs, levels, size), f32) for size in widths]
        + [pltpu.VMEM((levs - 1, pairs, levels, size), f32) for size in widths]
        + [pltpu.VMEM((tiles, levels * pairs, LANES), f32) for tiles in staged_tiles]
        + [
            pltpu.VMEM((8 * packs * slots, LANES), f32),
            pltpu.VMEM((waves - 1, 8, LANES), f32),
            pltpu.VMEM((waves, 8, LANES), f32),
            pltpu.VMEM((pairs, 8, LANES), f32),
            pltpu.VMEM((levs - 1, pairs, 8, LANES), f32),
            pltpu.VMEM((levs, 2 * modes_number, levels), bf16),
            pltpu.VMEM((2, levels, modes_number), bf16),
            dma((whole + 1,)),
            dma((chunks + 1,)),
            dma((chunks + 1,)),
            dma((chunks + 1, levs - 1)),
            dma((chunks + 1, levs - 1)),
            dma((whole + 1,)),
        ],
        compiler_params=pltpu.CompilerParams(
            collective_id=0, has_side_effects=True, vmem_limit_bytes=67043328
        ),
    )
    operands = (rows, last, to_modes, from_modes, depth[None, :])
    if waves == 4 * QUAD and levels % 2 == 0:
        half = waves // 2
        room = half * QUAD * 3 // 4
        int_shapes = [waves, groups, room, QUAD * groups, 1]
        picks, places, relayed, landed, fits = pl.pallas_call(
            functools.partial(tables, waves, groups, room),
            out_shape=[jax.ShapeDtypeStruct((size,), jnp.int32) for size in int_shapes],
            in_specs=[smem],
            out_specs=[smem] * 5,
            scratch_shapes=[pltpu.SMEM((4,), jnp.int32)],
        )(owner)
        solved = lax.cond(
            fits[0] > 0,
            lambda *given: relay_call(waves, levs, pairs, slots, levels, width, packs, rest, room, whole, modes_number)(*given),
            lambda one, two, three, four, *given: dense(one, two, *given),
            *(picks, places, relayed, landed, *operands),
        )
    else:
        numbers = jnp.arange(owner.shape[0], dtype=jnp.int32)
        mine = owner == own_index
        before = (numbers[:, None] > numbers[None, :]) & mine[None, :]
        rank = jnp.sum(before.astype(jnp.int32), axis=1)
        picks = jnp.sum(jnp.where(mine, rank, 0).reshape(waves, groups), axis=1)
        places = lax.dynamic_slice_in_dim(owner, own_index * groups, groups) ^ own_index
        solved = dense(picks, places, *operands)
    return solved.reshape(levels, pairs, (whole + 1) * LANES)[:, :, :width]


def solution(mesh):
    placed = (P("lev", "wave", None), P(), P(), P(), P())
    return jax.shard_map(
        per_device, mesh=mesh, in_specs=placed, out_specs=P("lev", "wave", None), check_vma=False
    )
```
